128 devices in a mesh: scale: 2 (over y_hi), lat: 64 (over x, z, y_lo, core).
Axes of the slice: x: 4, y: 4 (y_hi: 2, y_lo: 2; y = y_hi * 2 + y_lo), z: 4, core: 2. Of those that a mesh axis runs over, the one named last changes fastest.
Arguments:
- fine_state: float32 [64, 2, 1280, 1280], P(None, None, ('scale', 'lat')), may hold values from -6 to 6
- fine_noise: bfloat16 [64, 2, 1280, 1280], P(None, None, ('scale', 'lat')), may hold values from -6 to 6
- medium_state: float32 [64, 2, 640, 640], P(None, None, ('scale', 'lat')), may hold values from -6 to 6
- medium_noise: bfloat16 [64, 2, 640, 640], P(None, None, ('scale', 'lat')), may hold values from -6 to 6
- coarse_state: float32 [64, 2, 160, 160], P('lat'), may hold values from -6 to 6
- coarse_noise: bfloat16 [64, 2, 160, 160], P('lat'), may hold values from -6 to 6
- decay: float32 [3], replicated, may hold values from 0.5 to 0.95
- amplitude: float32 [3], replicated, may hold values from 0.3 to 1
- fine_basis: bfloat16 [1280, 128, 1280], P(('scale', 'lat')), may hold values from -0.0017089844 to 0.0017089844
- medium_basis: bfloat16 [640, 128, 640], P(('scale', 'lat')), may hold values from -0.0034179688 to 0.0034179688
- coarse_basis: bfloat16 [128, 160, 160], P(('scale', 'lat')), may hold values from -0.013671875 to 0.013671875
Outputs:
- fine_next: float32 [64, 2, 1280, 1280], P(None, None, ('scale', 'lat'))
- medium_next: float32 [64, 2, 640, 640], P(None, None, ('scale', 'lat'))
- coarse_next: float32 [64, 2, 160, 160], P('lat')
- pattern: float32 [64, 128, 2560], P(None, ('scale', 'lat'))
The draws below stay inside these ranges and needn't reach their ends.
All inputs are finite; a program needn't handle non-finite values.
Results may differ from the reference program's by a relative error of at most 0.005.
Values may be sent and summed in bfloat16 or wider, within the bound.
A program may use at most 128 MiB of HBM per device.

```python
import math
import jax
import jax.numpy as jnp
from jax import lax

MF = 1280
MM = 640
MC = 160
NLON = 2560
MEMBERS = 64
NROWS = 128


def shard_levels(own_key, dims, shards, smallest, largest):
    factor_of, own = 1.0, jax.random.fold_in(own_key, 6)
    for position, shards_of in shards:
        draws = jnp.exp(jax.random.uniform(jax.random.fold_in(own, position), (shards_of,), jnp.float32, smallest / len(shards), largest / len(shards)))
        factor_of = factor_of * jnp.repeat(draws, dims[position] // shards_of).reshape([-1 if axis == position else 1 for axis in range(len(dims))])
    return factor_of


def gaussian(own_key, dims, width, bound, pieces=(), held_as=jnp.bfloat16):
    factor_of = shard_levels(own_key, dims, pieces, -0.22, 0.18) if pieces else 1.0
    drawn = jax.random.normal(own_key, dims, jnp.float32) * width * factor_of
    return jnp.minimum(jnp.maximum(drawn, -bound), bound).astype(held_as)


def setup_inputs(seed: int = 0) -> dict:
    splits = jax.random.split(jax.random.key(seed), 12)
    fine_state = gaussian(splits[0], (MEMBERS, 2, MF, MF), 1.0, 6.0, ((2, 128),), jnp.float32)
    fine_noise = gaussian(splits[1], (MEMBERS, 2, MF, MF), 1.0, 6.0, ((2, 128),))
    medium_state = gaussian(splits[2], (MEMBERS, 2, MM, MM), 1.0, 6.0, ((2, 128),), jnp.float32)
    medium_noise = gaussian(splits[3], (MEMBERS, 2, MM, MM), 1.0, 6.0, ((2, 128),))
    coarse_state = gaussian(splits[4], (MEMBERS, 2, MC, MC), 1.0, 6.0, ((0, 64),), jnp.float32)
    coarse_noise = gaussian(splits[5], (MEMBERS, 2, MC, MC), 1.0, 6.0, ((0, 64),))
    decay = jnp.clip(jax.random.uniform(splits[6], (3,), jnp.float32, 0.5, 0.95), 0.5, 0.95)
    amplitude = jnp.clip(jax.random.uniform(splits[7], (3,), jnp.float32, 0.3, 1.0), 0.3, 1.0)
    fine_basis = gaussian(splits[8], (MF, NROWS, MF), (8 * MF * MF) ** -0.5, 0.0017089844, ((0, 128),))
    medium_basis = gaussian(splits[9], (MM, NROWS, MM), (8 * MM * MM) ** -0.5, 0.0034179688, ((0, 128),))
    coarse_basis = gaussian(splits[10], (NROWS, MC, MC), (8 * MC * MC) ** -0.5, 0.013671875, ((0, 128),))
    return {"fine_state": fine_state, "fine_noise": fine_noise, "medium_state": medium_state, "medium_noise": medium_noise, "coarse_state": coarse_state, "coarse_noise": coarse_noise, "decay": decay, "amplitude": amplitude, "fine_basis": fine_basis, "medium_basis": medium_basis, "coarse_basis": coarse_basis}


def advance(state, noise, decay_rate, amp_rate):
    slots = state.shape[3]
    mode_ids = jnp.arange(state.shape[2], dtype=jnp.int32)
    degree_ids = jnp.arange(slots, dtype=jnp.int32)
    inside = (mode_ids[:, None] + degree_ids[None, :]) < slots
    updated = decay_rate * state + amp_rate * noise.astype(jnp.float32)
    return jnp.where(inside, updated, jnp.zeros_like(updated))


def legendre_by_modes(half, basis):
    members, parts, modes, slots = half.shape
    nrow = basis.shape[1]
    blocks = modes // 32
    coef_blocks = jnp.moveaxis(half.reshape(members, parts, blocks, 32, slots), 2, 0)
    basis_blocks = basis.reshape(blocks, 32, nrow, slots)

    def one_block(pair):
        return jnp.einsum("ecmk,mrk->ecmr", pair[0].astype(jnp.float32), pair[1].astype(jnp.float32))

    result = lax.map(one_block, (coef_blocks, basis_blocks))
    return jnp.moveaxis(result, 0, 2).reshape(members, parts, modes, nrow)


def grid_table(modes):
    mode_ids = jnp.arange(modes, dtype=jnp.int32)
    lon_ids = jnp.arange(NLON, dtype=jnp.int32)
    angles = ((mode_ids[:, None] * lon_ids[None, :]) % NLON).astype(jnp.float32) * (2.0 * math.pi / NLON)
    weights = jnp.where(mode_ids == 0, 1.0, 2.0).astype(jnp.float32)[:, None]
    return jnp.stack([weights * jnp.cos(angles), -weights * jnp.sin(angles)]).astype(jnp.bfloat16)


def synthesis(fourier):
    table = grid_table(fourier.shape[2])
    return jnp.einsum("ecmr,cml->erl", fourier.astype(jnp.float32), table.astype(jnp.float32))


def reference(fine_state, fine_noise, medium_state, medium_noise, coarse_state, coarse_noise, decay, amplitude, fine_basis, medium_basis, coarse_basis):
    fine_next = advance(fine_state, fine_noise, decay[0], amplitude[0])
    medium_next = advance(medium_state, medium_noise, decay[1], amplitude[1])
    coarse_next = advance(coarse_state, coarse_noise, decay[2], amplitude[2])
    fine_fourier = legendre_by_modes(fine_next.astype(jnp.bfloat16), fine_basis).astype(jnp.bfloat16)
    medium_fourier = legendre_by_modes(medium_next.astype(jnp.bfloat16), medium_basis).astype(jnp.bfloat16)
    coarse_fourier = jnp.einsum("ecmk,rmk->ecmr", coarse_next.astype(jnp.bfloat16).astype(jnp.float32), coarse_basis.astype(jnp.float32)).astype(jnp.bfloat16)
    total = synthesis(fine_fourier) + synthesis(medium_fourier) + synthesis(coarse_fourier)
    pattern = jnp.tanh(total).astype(jnp.float32)
    return fine_next, medium_next, coarse_next, pattern
```

```python
import math

import jax
import jax.numpy as jnp
import numpy as np
from jax import lax
from jax.experimental import pallas as pl
from jax.experimental.pallas import tpu as pltpu
from jax.sharding import PartitionSpec as P

MESH = pl.DeviceIdType.MESH
F32, BF16 = jnp.float32, jnp.bfloat16
ANY = pl.BlockSpec(memory_space=pl.ANY)
HBM = pl.BlockSpec(memory_space=pltpu.HBM)
VMEM = pl.BlockSpec(memory_space=pltpu.VMEM)
SMEM = pl.BlockSpec(memory_space=pltpu.SMEM)
MF, MM, MC, NLON, NE, NR = 1280, 640, 160, 2560, 64, 128
ND = 128
OWNERS = 32
TWO_TILES = 7
NT = (((1,), (1,)), ((), ()))


def my_place():
    return lax.axis_index("scale") * 64 + lax.axis_index("lat")


def to_device(d):
    return (d // 64, d % 64)


def coarse_kernel(cs, cn, cb, dec, amp, nxt, h0, h1, b0, b1, pad, bpad):
    scale = lax.axis_index("scale")
    deg = lax.broadcasted_iota(jnp.int32, (MC, MC), 0) + lax.broadcasted_iota(jnp.int32, (MC, MC), 1)
    for c in range(2):
        val = dec[2] * cs[0, c] + amp[2] * cn[0, c].astype(F32)
        val = jnp.where(deg < MC, val, 0.0)
        nxt[0, c] = val
    pad[pl.ds(160, 8), :] = jnp.zeros((8, 256), F32)
    bpad[pl.ds(160, 8), :] = jnp.zeros((8, 256), F32)
    pad[pl.ds(0, 160), pl.ds(128, 128)] = jnp.zeros((160, 128), F32)
    bpad[pl.ds(0, 160), pl.ds(128, 128)] = jnp.zeros((160, 128), F32)
    pad[pl.ds(0, 160), pl.ds(0, 160)] = nxt[0, scale]
    bpad[pl.ds(0, 160), pl.ds(0, 160)] = cb[0].astype(F32)
    for p in range(OWNERS):
        h0[p] = pad[pl.ds(5 * p, 8), pl.ds(0, 128)].astype(BF16)
        b0[p] = bpad[pl.ds(5 * p, 8), pl.ds(0, 128)].astype(BF16)
        if p < TWO_TILES:
            h1[p] = pad[pl.ds(5 * p, 8), pl.ds(128, 128)].astype(BF16)
            b1[p] = bpad[pl.ds(5 * p, 8), pl.ds(128, 128)].astype(BF16)


def coarse_call(cs, cn, cb, dec, amp):
    s = jax.ShapeDtypeStruct
    return pl.pallas_call(
        coarse_kernel,
        name="coarse_advance",
        out_shape=(
            s((1, 2, MC, MC), F32),
            s((OWNERS, 8, 128), BF16),
            s((TWO_TILES, 8, 128), BF16),
            s((OWNERS, 8, 128), BF16),
            s((TWO_TILES, 8, 128), BF16),
        ),
        in_specs=[VMEM, VMEM, VMEM, SMEM, SMEM],
        out_specs=(VMEM,) * 5,
        scratch_shapes=[pltpu.VMEM((168, 256), F32), pltpu.VMEM((168, 256), F32)],
        cost_estimate=pl.CostEstimate(flops=10**6, bytes_accessed=10**6, transcendentals=0),
    )(cs, cn, cb, dec, amp)


def reshard_kernel(h0, h1, b0, b1, rh0, rh1, rb0, rb1, send, recv_h, recv_b, here):
    me = my_place()

    def go(i, tops, k, sent):
        p = lax.rem(me + i, tops)
        tiles = ((h0, rh0, recv_h), (b0, rb0, recv_b)) if k == 0 else ((h1, rh1, recv_h), (b1, rb1, recv_b))

        @pl.when(p != me)
        def _():
            for src, dst, sem in tiles:
                pltpu.make_async_remote_copy(
                    src.at[p], dst.at[me], send.at[k], sem.at[k], device_id=to_device(p), device_id_type=MESH
                ).start()

        @pl.when(p == me)
        def _():
            for src, dst, _ in tiles:
                pltpu.make_async_copy(src.at[p], dst.at[me], here.at[k]).start()

    @pl.loop(0, OWNERS)
    def _(i):
        go(i, OWNERS, 0, send)

    @pl.loop(0, TWO_TILES)
    def _(i):
        go(i, TWO_TILES, 1, send)

    def wait(count, sem):
        part = rh0.at[pl.ds(0, count)]
        pltpu.make_async_copy(part, part, sem).wait()

    for k, tops in ((0, OWNERS), (1, TWO_TILES)):

        @pl.when(me < tops)
        def _():
            wait(2 * tops - 2, send.at[k])
            wait(2, here.at[k])
            wait(ND - 1, recv_h.at[k])
            wait(ND - 1, recv_b.at[k])

        @pl.when(me >= tops)
        def _():
            wait(2 * tops, send.at[k])


def reshard_call(h0, h1, b0, b1):
    s = jax.ShapeDtypeStruct((ND, 8, 128), BF16)
    return pl.pallas_call(
        reshard_kernel,
        name="coarse_reshard",
        out_shape=(s, s, s, s),
        in_specs=[HBM] * 4,
        out_specs=(ANY,) * 4,
        scratch_shapes=[pltpu.SemaphoreType.DMA((2,))] * 4,
        compiler_params=pltpu.CompilerParams(has_side_effects=True, vmem_limit_bytes=67_000_000),
        cost_estimate=pl.CostEstimate(flops=10**6, bytes_accessed=10**6, transcendentals=0),
    )(h0, h1, b0, b1)


BLOCKS = [(0, 0), (0, 1), (1, 0), (1, 1), (2, 0)]


def spectral_kernel(
    fs, fn, ms, mn, fb, mb, rh0, rh1, rb0, rb1, dec, amp,
    fo, mo, g,
    s_buf, n_buf, fb_buf, mb_buf, a_buf, acc, gf, c_raw, hf, bf,
    s_sem, n_sem, b_sem, o_sem, c_sem,
):
    me = my_place()
    order = [4, 0, 1, 2, 3]

    def start_copies(u, kt, out):
        grp, q = BLOCKS[u]
        lanes = pl.ds((q * 5 + kt) * 128, 128)
        rows = s_buf.at[u].reshape(5 * 64, 5, 2, 128).at[pl.ds(kt * 64, 64)]
        nrows = n_buf.at[u, pl.ds(kt * 64, 64)]
        if grp == 2:
            src, nsrc, dst = ms, mn, mo
            mid = slice(None)
        else:
            src, nsrc, dst = fs, fn, fo
            mid = pl.ds(grp * 5, 5)
        if out:
            pltpu.make_async_copy(rows, dst.at[:, mid, :, lanes], o_sem.at[u]).start()
        else:
            pltpu.make_async_copy(src.at[:, mid, :, lanes], rows, s_sem.at[u]).start()
            pltpu.make_async_copy(nsrc.at[:, mid, :, lanes], nrows, n_sem.at[u]).start()

    basis = [
        pltpu.make_async_copy(fb.at[pl.ds(0, 5)], fb_buf.at[pl.ds(0, 5)], b_sem.at[0]),
        pltpu.make_async_copy(fb.at[pl.ds(5, 5)], fb_buf.at[pl.ds(5, 5)], b_sem.at[1]),
        pltpu.make_async_copy(mb, mb_buf, b_sem.at[2]),
    ]
    started = set()
    for u in order:
        for kt in range(5):
            start_copies(u, kt, False)
        grp = BLOCKS[u][0]
        if grp not in started:
            started.add(grp)
            basis[grp].start()

    @pl.when(me < OWNERS)
    def _():
        pltpu.make_async_copy(rh0, c_raw.at[0], c_sem.at[0]).start()
        pltpu.make_async_copy(rb0, c_raw.at[1], c_sem.at[0]).start()

        @pl.when(me < TWO_TILES)
        def _():
            pltpu.make_async_copy(rh1, c_raw.at[2], c_sem.at[1]).start()
            pltpu.make_async_copy(rb1, c_raw.at[3], c_sem.at[1]).start()

    rows80 = lax.broadcasted_iota(jnp.int32, (40, 128), 0)
    lane = lax.broadcasted_iota(jnp.int32, (40, 128), 1)
    deg = lax.div(lax.rem(rows80, 10), 2) + lane

    gf[...] = jnp.zeros_like(gf)
    done = set()
    for u in order:
        grp, q = BLOCKS[u]
        which = 1 if grp == 2 else 0
        size = MM if grp == 2 else MF
        first = me * 5 if grp == 2 else me * 10 + grp * 5
        d, a = dec[which], amp[which]
        pltpu.make_async_copy(s_buf.at[u], s_buf.at[u], s_sem.at[u]).wait()
        pltpu.make_async_copy(n_buf.at[u], n_buf.at[u], n_sem.at[u]).wait()
        for kt in range(5):
            inside = deg < size - first - (q * 5 + kt) * 128
            inside = jnp.concatenate([inside, inside], axis=0)

            @pl.loop(0, 8)
            def _(j):
                r = pl.ds(pl.multiple_of(kt * 640 + j * 80, 80), 80)
                val = d * s_buf[u, r, :] + a * n_buf.at[u].reshape(3200, 128)[r, :].astype(F32)
                s_buf[u, r, :] = jnp.where(inside, val, 0.0)

            start_copies(u, kt, True)
            for m in range(5):
                for c in range(2):
                    v = s_buf[u, pl.ds(kt * 640 + m * 2 + c, 64, stride=10), :]
                    a_buf[m, pl.ds(c * 64, 64), pl.ds(kt * 128, 128)] = v.astype(BF16)
        if grp not in done:
            done.add(grp)
            basis[grp].wait()
        for m in range(5):
            if grp == 2:
                b = mb_buf[m]
            else:
                b = fb_buf[grp * 5 + m, :, pl.ds(q * 640, 640)]
            out = lax.dot_general(b, a_buf[m], NT, preferred_element_type=F32)
            if grp < 2 and q == 0:
                acc[m] = out
            else:
                if grp < 2:
                    out = out + acc[m]
                gf[pl.ds(grp * 5 + m, 128, stride=16), :] = out.astype(BF16).astype(F32)

    @pl.when(me < OWNERS)
    def _():
        pltpu.make_async_copy(c_raw.at[pl.ds(0, 2)], c_raw.at[pl.ds(0, 2)], c_sem.at[0]).wait()

        @pl.when(me < TWO_TILES)
        def _():
            pltpu.make_async_copy(c_raw.at[pl.ds(2, 2)], c_raw.at[pl.ds(2, 2)], c_sem.at[1]).wait()

        def add(base, first_time):
            hf[...] = c_raw[base].reshape(1024, 128).astype(F32)
            bf[...] = c_raw[base + 1].reshape(1024, 128).astype(F32)
            for m in range(5):
                h = hf[pl.ds(m, 128, stride=8), :].astype(BF16)
                b = bf[pl.ds(m, 128, stride=8), :].astype(BF16)
                out = lax.dot_general(b, h, NT, preferred_element_type=F32)
                acc[m] = out if first_time else acc[m] + out

        add(0, True)

        @pl.when(me < TWO_TILES)
        def _():
            add(2, False)

        for m in range(5):
            r = pl.ds(10 + m, 128, stride=16)
            gf[r, :] = gf[r, :] + acc[m].astype(BF16).astype(F32)

    g[...] = gf[...].astype(BF16).reshape(128, 16, 128)
    for u in range(5):
        pltpu.make_async_copy(s_buf.at[u], s_buf.at[u], o_sem.at[u]).wait()


def spectral_call(fs, fn, ms, mn, fb, mb, rh0, rh1, rb0, rb1, dec, amp):
    s = jax.ShapeDtypeStruct
    dma = pltpu.SemaphoreType.DMA
    return pl.pallas_call(
        spectral_kernel,
        name="spectral",
        out_shape=(s((NE, 10, 2, MF), F32), s((NE, 5, 2, MM), F32), s((ND, 16, 128), BF16)),
        in_specs=[HBM] * 6 + [ANY] * 4 + [SMEM] * 2,
        out_specs=(HBM, HBM, VMEM),
        scratch_shapes=[
            pltpu.VMEM((5, 3200, 128), F32),
            pltpu.VMEM((5, 320, 5, 2, 128), BF16),
            pltpu.VMEM((10, 128, MF), BF16),
            pltpu.VMEM((5, 128, MM), BF16),
            pltpu.VMEM((5, 128, 640), BF16),
            pltpu.VMEM((5, 128, 128), F32),
            pltpu.VMEM((2048, 128), F32),
            pltpu.VMEM((4, 128, 8, 128), BF16),
            pltpu.VMEM((1024, 128), F32),
            pltpu.VMEM((1024, 128), F32),
            dma((5,)),
            dma((5,)),
            dma((3,)),
            dma((5,)),
            dma((2,)),
        ],
        compiler_params=pltpu.CompilerParams(vmem_limit_bytes=67_000_000),
        cost_estimate=pl.CostEstimate(flops=10**9, bytes_accessed=25 * 10**6, transcendentals=0),
    )(fs, fn, ms, mn, fb, mb, rh0, rh1, rb0, rb1, dec, amp)


def exchange_kernel(g, out, send, recv, here):
    me = my_place()
    own = pltpu.make_async_copy(g.at[me], out.at[me], here)
    own.start()

    @pl.loop(1, ND)
    def _(i):
        d = lax.rem(me + i, ND)
        pltpu.make_async_remote_copy(
            g.at[d], out.at[me], send, recv, device_id=to_device(d), device_id_type=MESH
        ).start()

    own.wait()
    part = out.at[pl.ds(0, ND - 1)]
    pltpu.make_async_copy(part, part, send).wait()
    pltpu.make_async_copy(part, part, recv).wait()


def exchange_call(g):
    return pl.pallas_call(
        exchange_kernel,
        name="exchange",
        out_shape=jax.ShapeDtypeStruct((ND, 16, 128), BF16),
        in_specs=[HBM],
        out_specs=ANY,
        scratch_shapes=[pltpu.SemaphoreType.DMA(())] * 3,
        compiler_params=pltpu.CompilerParams(has_side_effects=True, vmem_limit_bytes=8 * 2**20),
        cost_estimate=pl.CostEstimate(flops=10**6, bytes_accessed=10**6, transcendentals=0),
    )(g)


def synthesis_kernel(rec, w, tw, pat, rf, x, y, pv, sem):
    rf[...] = rec[...].reshape(2048, 128).astype(F32)
    for i in range(10):
        f = rf[pl.ds(i, 128, stride=16), :]
        med = rf[pl.ds(10 + i % 5 + 16 * (i // 5), 64, stride=32), :]
        f = jnp.concatenate([f[:64] + med, f[64:]], axis=0)
        if i == 0:
            row = lax.broadcasted_iota(jnp.int32, (128, 128), 0)
            f = jnp.where(row == 0, f, 2.0 * f)
        else:
            f = 2.0 * f
        t = f.T.astype(BF16)
        x[pl.ds(i * 64, 64), pl.ds(0, 128)] = t[:64]
        x[pl.ds(i * 64, 64), pl.ds(128, 128)] = t[64:]
    y[...] = jnp.dot(x[...], w[...], preferred_element_type=F32)
    view = pv.reshape(20 * 64, 1, 128)
    for half in range(2):
        for j in range(5):
            col = pl.ds(j * 256 + half * 128, 128)
            parts = [None, None]
            for i in range(10):
                yr = y[pl.ds(i * 64, 64), pl.ds(half * 128, 128)]
                if i == 0:
                    term = yr
                else:
                    yi = y[pl.ds(i * 64, 64), pl.ds(256 + half * 128, 128)]
                    term = tw[pl.ds(i, 1), col] * yr - tw[pl.ds(16 + i, 1), col] * yi
                k = i % 2
                parts[k] = term if parts[k] is None else parts[k] + term
            for k, val in ((0, parts[0] + parts[1]), (5, parts[0] - parts[1])):
                lt = (j + k) * 2 + half
                pv[pl.ds(lt * 64, 64), :] = jnp.tanh(val)
                pltpu.make_async_copy(view.at[pl.ds(lt * 64, 64)], pat.at[:, :, pl.ds(lt * 128, 128)], sem).start()
    pltpu.make_async_copy(pv, pv, sem).wait()


def synthesis_call(rec):
    p = np.arange(128)[:, None]
    ang = 2.0 * math.pi * ((p * np.arange(256)[None, :]) % 256) / 256.0
    c, s = np.cos(ang), np.sin(ang)
    w = jnp.asarray(np.block([[c, s], [-s, c]]), BF16)
    i = np.arange(16)[:, None]
    ang = 2.0 * math.pi * ((i * np.arange(1280)[None, :]) % NLON) / NLON
    tw = jnp.asarray(np.concatenate([np.cos(ang), np.sin(ang)]), F32)
    return pl.pallas_call(
        synthesis_kernel,
        name="synthesis",
        out_shape=jax.ShapeDtypeStruct((NE, 1, NLON), F32),
        in_specs=[VMEM] * 3,
        out_specs=HBM,
        scratch_shapes=[
            pltpu.VMEM((2048, 128), F32),
            pltpu.VMEM((640, 256), BF16),
            pltpu.VMEM((640, 512), F32),
            pltpu.VMEM((1280, 128), F32),
            pltpu.SemaphoreType.DMA(()),
        ],
        compiler_params=pltpu.CompilerParams(vmem_limit_bytes=20 * 2**20),
        cost_estimate=pl.CostEstimate(flops=10**8, bytes_accessed=10**6, transcendentals=0),
    )(rec, w, tw)


def body(fs, fn, ms, mn, cs, cn, decay, amplitude, fb, mb, cb):
    fs, fn, ms, mn = (a.transpose(0, 2, 1, 3) for a in (fs, fn, ms, mn))
    coarse_next, h0, h1, b0, b1 = coarse_call(cs, cn, cb, decay, amplitude)
    rh0, rh1, rb0, rb1 = reshard_call(h0, h1, b0, b1)
    fine_next, medium_next, g = spectral_call(fs, fn, ms, mn, fb, mb, rh0, rh1, rb0, rb1, decay, amplitude)
    rec = exchange_call(g)
    pattern = synthesis_call(rec)
    return (fine_next.transpose(0, 2, 1, 3), medium_next.transpose(0, 2, 1, 3), coarse_next, pattern)


def solution(mesh):
    both = ("scale", "lat")
    return jax.shard_map(
        body,
        mesh=mesh,
        in_specs=(
            P(None, None, both, None),
            P(None, None, both, None),
            P(None, None, both, None),
            P(None, None, both, None),
            P("lat", None, None, None),
            P("lat", None, None, None),
            P(),
            P(),
            P(both, None, None),
            P(both, None, None),
            P(both, None, None),
        ),
        out_specs=(
            P(None, None, both, None),
            P(None, None, both, None),
            P("lat", None, None, None),
            P(None, both, None),
        ),
        check_vma=False,
    )
```

```python
import math

import jax
import jax.numpy as jnp
import numpy as np
from jax import lax
from jax.experimental import pallas as pl
from jax.experimental.pallas import tpu as pltpu
from jax.sharding import PartitionSpec as P

MESH = pl.DeviceIdType.MESH
F32, BF16 = jnp.float32, jnp.bfloat16
HBM = pl.BlockSpec(memory_space=pltpu.HBM)
VMEM = pl.BlockSpec(memory_space=pltpu.VMEM)
SMEM = pl.BlockSpec(memory_space=pltpu.SMEM)
MF, MM, MC, NLON, NE, NR = 1280, 640, 160, 2560, 64, 128
ND = 128
NT = (((1,), (1,)), ((), ()))


def my_place():
    return lax.axis_index("scale") * 64 + lax.axis_index("lat")


def to_device(d):
    return (d // 64, d % 64)

BLOCKS = [(0, 0), (0, 1), (2, 0), (1, 0), (1, 1)]
STEP = 37


def send_all(me, src, dst, send, recv, here):
    pltpu.make_async_copy(src.at[me], dst.at[me], here).start()

    @pl.loop(1, ND)
    def _(i):
        d = lax.rem(me + i * STEP, ND)
        pltpu.make_async_remote_copy(
            src.at[d], dst.at[me], send, recv, device_id=to_device(d), device_id_type=MESH
        ).start()


def wait_rows(ref, count, sem):
    part = ref.at[pl.ds(0, count)]
    pltpu.make_async_copy(part, part, sem).wait()


def spectral_kernel(
    fs, fn, ms, mn, fb, mb, cs, cn, cb, dec, amp,
    s_buf, c_next, r1, r2, r3, rx,
    n_buf, n_flat, fb_buf, mb_buf, a_buf, acc, stage, g1, g2, g3, gx,
    cs_buf, cn_buf, cb_buf, pad, c_stage, c_msg, c_got,
    s_sem, n_sem, b_sem, c_sem, send, recv, here,
):
    me = my_place()
    scale = lax.axis_index("scale")

    coarse_in = (
        pltpu.make_async_copy(cs, cs_buf, c_sem.at[0]),
        pltpu.make_async_copy(cn, cn_buf, c_sem.at[1]),
        pltpu.make_async_copy(cb, cb_buf, c_sem.at[2]),
    )
    for copy in coarse_in:
        copy.start()

    basis = [
        pltpu.make_async_copy(fb.at[pl.ds(0, 5)], fb_buf.at[pl.ds(0, 5)], b_sem.at[0]),
        pltpu.make_async_copy(fb.at[pl.ds(5, 5)], fb_buf.at[pl.ds(5, 5)], b_sem.at[1]),
        pltpu.make_async_copy(mb, mb_buf, b_sem.at[2]),
    ]
    started = set()
    for u, (grp, q) in enumerate(BLOCKS):
        for kt in range(5):
            lanes = pl.ds((q * 5 + kt) * 128, 128)
            rows = s_buf.at[u].reshape(5 * 64, 5, 2, 128).at[pl.ds(kt * 64, 64)]
            if grp == 2:
                src, nsrc, mid = ms, mn, slice(None)
            else:
                src, nsrc, mid = fs, fn, pl.ds(grp * 5, 5)
            pltpu.make_async_copy(src.at[:, mid, :, lanes], rows, s_sem.at[u]).start()
            pltpu.make_async_copy(nsrc.at[:, mid, :, lanes], n_buf.at[u, pl.ds(kt * 64, 64)], n_sem.at[u]).start()
        if grp not in started:
            started.add(grp)
            basis[grp].start()

    barrier = pltpu.get_barrier_semaphore()

    @pl.loop(1, ND)
    def _(i):
        d = lax.rem(me + i * STEP, ND)
        pl.semaphore_signal(barrier, inc=1, device_id=to_device(d), device_id_type=MESH)

    for copy in coarse_in:
        copy.wait()
    cdeg = lax.broadcasted_iota(jnp.int32, (MC, MC), 0) + lax.broadcasted_iota(jnp.int32, (MC, MC), 1)
    for c in range(2):
        val = dec[2] * cs_buf[0, c] + amp[2] * cn_buf[0, c].astype(F32)
        c_next[0, c] = jnp.where(cdeg < MC, val, 0.0)
    pad[...] = jnp.zeros_like(pad)
    pad[0, :, pl.ds(0, MC)] = c_next[0, scale]
    pad[1, :, pl.ds(0, MC)] = cb_buf[0].astype(F32)
    for k in range(2):
        c_stage[pl.ds(2 * k, 128, stride=4), :] = pad[k, pl.ds(0, 128), pl.ds(0, 128)]
        extra = jnp.concatenate(
            [pad[k, pl.ds(0, 32), pl.ds(128, 128)], pad[k, pl.ds(128, 32), pl.ds(0, 128)], jnp.zeros((64, 128), F32)], axis=0
        )
        c_stage[pl.ds(2 * k + 1, 128, stride=4), :] = extra
    c_msg.reshape(512, 128)[...] = c_stage[...].astype(BF16)

    pl.semaphore_wait(barrier, ND - 1)
    send_all(me, c_msg, c_got, send.at[3], recv.at[3], here.at[3])

    rows40 = lax.broadcasted_iota(jnp.int32, (40, 128), 0)
    deg = lax.div(lax.rem(rows40, 10), 2) + lax.broadcasted_iota(jnp.int32, (40, 128), 1)

    def advance(u, kt):
        grp, q = BLOCKS[u]
        which = 1 if grp == 2 else 0
        size = MM if grp == 2 else MF
        first = me * 5 if grp == 2 else me * 10 + grp * 5
        d, a = dec[which], amp[which]
        inside = deg < size - first - (q * 5 + kt) * 128
        inside = jnp.concatenate([inside, inside], axis=0)

        @pl.loop(0, 8)
        def _(j):
            r = pl.ds(pl.multiple_of(kt * 640 + j * 80, 80), 80)
            n_flat[...] = n_buf.at[u].reshape(3200, 128)[r, :]
            val = d * s_buf[u, r, :] + a * n_flat[...].astype(F32)
            s_buf[u, r, :] = jnp.where(inside, val, 0.0)

        for m in range(5):
            for c in range(2):
                v = s_buf[u, pl.ds(kt * 640 + m * 2 + c, 64, stride=10), :]
                a_buf[m, pl.ds(c * 64, 64), pl.ds(kt * 128, 128)] = v.astype(BF16)

    def legendre(u, put):
        grp, q = BLOCKS[u]
        for m in range(5):
            b = mb_buf[m] if grp == 2 else fb_buf[grp * 5 + m, :, pl.ds(q * 640, 640)]
            out = lax.dot_general(b, a_buf[m], NT, preferred_element_type=F32)
            if grp < 2 and q == 0:
                acc[m] = out
            else:
                put(m, out + acc[m] if grp < 2 else out)

    def begin(u):
        pltpu.make_async_copy(s_buf.at[u], s_buf.at[u], s_sem.at[u]).wait()
        pltpu.make_async_copy(n_buf.at[u], n_buf.at[u], n_sem.at[u]).wait()

    def block(u, put, after_first=None):
        begin(u)
        for kt in range(5):
            advance(u, kt)
            if kt == 0 and after_first is not None:
                after_first()
        if BLOCKS[u][1] == 0:
            basis[BLOCKS[u][0]].wait()
        legendre(u, put)

    def put_first(m, out):
        if m < 4:
            stage[pl.ds(m, 128, stride=4), :] = out
        else:
            acc[0] = out

    block(0, None)
    block(1, put_first)
    g1.reshape(512, 128)[...] = stage[pl.ds(0, 512), :].astype(BF16)
    stage[pl.ds(0, 128, stride=6), :] = acc[0]

    def put_medium(m, out):
        stage[pl.ds(1 + m, 128, stride=6), :] = out

    block(2, put_medium, lambda: send_all(me, g1, r1, send.at[0], recv.at[0], here.at[0]))
    g2.reshape(768, 128)[...] = stage[...].astype(BF16)
    block(3, None, lambda: send_all(me, g2, r2, send.at[1], recv.at[1], here.at[1]))

    wait_rows(c_got, ND - 1, recv.at[3])
    pltpu.make_async_copy(c_got.at[me], c_got.at[me], here.at[3]).wait()
    c_stage[...] = c_got.reshape(512, 128)[...].astype(F32)
    part = [c_stage[pl.ds(k, 128, stride=4), :].astype(BF16) for k in range(4)]
    main = lax.dot_general(part[2], part[0], NT, preferred_element_type=F32)
    extra = lax.dot_general(part[3], part[1], NT, preferred_element_type=F32)
    stage[pl.ds(5, 128, stride=6), :] = main + jnp.where(me < 32, extra, 0.0)
    c_stage[pl.ds(0, 128, stride=2), :] = extra
    c_stage[pl.ds(1, 128, stride=2), :] = jnp.zeros((128, 128), F32)
    gx.reshape(256, 128)[...] = c_stage[pl.ds(0, 256), :].astype(BF16)
    wide = jnp.logical_and(me >= 32, me < 64)
    slot = lax.rem(me, 32)

    def send_extra():
        @pl.when(wide)
        def _():
            pltpu.make_async_copy(gx.at[me], rx.at[slot], here.at[4]).start()

            @pl.loop(1, ND)
            def _(i):
                d = lax.rem(me + i * STEP, ND)
                pltpu.make_async_remote_copy(
                    gx.at[d], rx.at[slot], send.at[4], recv.at[4], device_id=to_device(d), device_id_type=MESH
                ).start()

    def put_last(m, out):
        stage[pl.ds(m, 128, stride=6), :] = out

    block(4, put_last, send_extra)
    g3.reshape(768, 128)[...] = stage[...].astype(BF16)
    send_all(me, g3, r3, send.at[2], recv.at[2], here.at[2])

    wait_rows(c_got, ND - 1, send.at[3])

    @pl.when(wide)
    def _():
        pltpu.make_async_copy(gx.at[0], rx.at[0], here.at[4]).wait()
        wait_rows(gx, ND - 1, send.at[4])
        wait_rows(rx, 31, recv.at[4])

    @pl.when(jnp.logical_not(wide))
    def _():
        wait_rows(rx, 32, recv.at[4])

    for k, r in enumerate((r1, r2, r3)):
        pltpu.make_async_copy(r.at[0], r.at[0], here.at[k]).wait()
        wait_rows(r, ND - 1, send.at[k])
        wait_rows(r, ND - 1, recv.at[k])


def spectral_call(fs, fn, ms, mn, fb, mb, cs, cn, cb, dec, amp):
    dma = pltpu.SemaphoreType.DMA
    v = pltpu.VMEM
    return pl.pallas_call(
        spectral_kernel,
        name="spectral",
        out_shape=(
            v((5, 3200, 128), F32),
            v((1, 2, MC, MC), F32),
            v((ND, 2, 2, 128), BF16),
            v((ND, 3, 2, 128), BF16),
            v((ND, 3, 2, 128), BF16),
            v((32, 2, 128), BF16),
        ),
        in_specs=[HBM] * 9 + [SMEM] * 2,
        out_specs=(VMEM,) * 6,
        scratch_shapes=[
            v((5, 320, 5, 2, 128), BF16),
            v((80, 128), BF16),
            v((10, 128, MF), BF16),
            v((5, 128, MM), BF16),
            v((5, 128, 640), BF16),
            v((5, 128, 128), F32),
            v((768, 128), F32),
            v((ND, 2, 2, 128), BF16),
            v((ND, 3, 2, 128), BF16),
            v((ND, 3, 2, 128), BF16),
            v((ND, 2, 128), BF16),
            v((1, 2, MC, MC), F32),
            v((1, 2, MC, MC), BF16),
            v((1, MC, MC), BF16),
            v((2, MC, 256), F32),
            v((512, 128), F32),
            v((ND, 4, 128), BF16),
            v((ND, 4, 128), BF16),
            dma((5,)),
            dma((5,)),
            dma((3,)),
            dma((3,)),
            dma((5,)),
            dma((5,)),
            dma((5,)),
        ],
        compiler_params=pltpu.CompilerParams(has_side_effects=True, collective_id=0, vmem_limit_bytes=30 * 2**20),
        cost_estimate=pl.CostEstimate(flops=10**9, bytes_accessed=25 * 10**6, transcendentals=0),
    )(fs, fn, ms, mn, fb, mb, cs, cn, cb, dec, amp)


def synthesis_kernel(s_buf, c_next, r1, r2, r3, rx, w, tw, fo, mo, co, pat, f1, f2, f3, cf, x, y, pv, o_sem, c_sem, p_sem):
    for u, (grp, q) in enumerate(BLOCKS):
        for kt in range(5):
            rows = s_buf.at[u].reshape(5 * 64, 5, 2, 128).at[pl.ds(kt * 64, 64)]
            dst, mid = (mo, slice(None)) if grp == 2 else (fo, pl.ds(grp * 5, 5))
            pltpu.make_async_copy(rows, dst.at[:, mid, :, pl.ds((q * 5 + kt) * 128, 128)], o_sem).start()
    coarse_out = pltpu.make_async_copy(c_next, co, c_sem)
    coarse_out.start()

    f1[...] = r1.reshape(512, 128)[...].astype(F32)
    f2[...] = r2.reshape(768, 128)[...].astype(F32)
    f3[...] = r3.reshape(768, 128)[...].astype(F32)
    cf[pl.ds(0, 128), :] = f3[pl.ds(5, 128, stride=6), :]
    y[pl.ds(0, 64), pl.ds(0, 128)] = rx.reshape(64, 128)[...].astype(F32)
    cf[pl.ds(128, 32), :] = y[pl.ds(0, 64), pl.ds(0, 128)].reshape(32, 2, 128)[:, 0, :]
    for i in range(10):
        if i < 4:
            f = f1[pl.ds(i, 128, stride=4), :]
        elif i == 4:
            f = f2[pl.ds(0, 128, stride=6), :]
        else:
            f = f3[pl.ds(i - 5, 128, stride=6), :]
        med = f2[pl.ds(1 + i % 5 + 6 * (i // 5), 64, stride=12), :]
        coarse = cf[pl.ds(i, 16, stride=10), :]
        f = jnp.concatenate([f[:16] + (med[:16] + coarse), f[16:64] + med[16:], f[64:]], axis=0)
        if i == 0:
            row = lax.broadcasted_iota(jnp.int32, (128, 128), 0)
            f = jnp.where(row == 0, f, 2.0 * f)
        else:
            f = 2.0 * f
        t = f.T.astype(BF16)
        x[pl.ds(i * 64, 64), pl.ds(0, 128)] = t[:64]
        x[pl.ds(i * 64, 64), pl.ds(128, 128)] = t[64:]
    y[...] = jnp.dot(x[...], w[...], preferred_element_type=F32)
    view = pv.reshape(20 * 64, 1, 128)
    for half in range(2):
        for j in range(5):
            col = pl.ds(j * 256 + half * 128, 128)
            parts = [None, None]
            for i in range(10):
                yr = y[pl.ds(i * 64, 64), pl.ds(half * 128, 128)]
                if i == 0:
                    term = yr
                else:
                    yi = y[pl.ds(i * 64, 64), pl.ds(256 + half * 128, 128)]
                    term = tw[pl.ds(i, 1), col] * yr - tw[pl.ds(16 + i, 1), col] * yi
                k = i % 2
                parts[k] = term if parts[k] is None else parts[k] + term
            for k, val in ((0, parts[0] + parts[1]), (5, parts[0] - parts[1])):
                lt = (j + k) * 2 + half
                pv[pl.ds(lt * 64, 64), :] = jnp.tanh(val)
                pltpu.make_async_copy(view.at[pl.ds(lt * 64, 64)], pat.at[:, :, pl.ds(lt * 128, 128)], p_sem).start()
    pltpu.make_async_copy(s_buf, s_buf, o_sem).wait()
    coarse_out.wait()
    pltpu.make_async_copy(pv, pv, p_sem).wait()


def synthesis_call(*parts):
    p = np.arange(128)[:, None]
    ang = 2.0 * math.pi * ((p * np.arange(256)[None, :]) % 256) / 256.0
    c, s = np.cos(ang), np.sin(ang)
    w = jnp.asarray(np.block([[c, s], [-s, c]]), BF16)
    i = np.arange(16)[:, None]
    ang = 2.0 * math.pi * ((i * np.arange(1280)[None, :]) % NLON) / NLON
    tw = jnp.asarray(np.concatenate([np.cos(ang), np.sin(ang)]), F32)
    s = jax.ShapeDtypeStruct
    v = pltpu.VMEM
    return pl.pallas_call(
        synthesis_kernel,
        name="synthesis",
        out_shape=(
            s((NE, 10, 2, MF), F32),
            s((NE, 5, 2, MM), F32),
            s((1, 2, MC, MC), F32),
            s((NE, 1, NLON), F32),
        ),
        in_specs=[VMEM] * 8,
        out_specs=(HBM,) * 4,
        scratch_shapes=[
            v((512, 128), F32),
            v((768, 128), F32),
            v((768, 128), F32),
            v((160, 128), F32),
            v((640, 256), BF16),
            v((640, 512), F32),
            v((1280, 128), F32),
            pltpu.SemaphoreType.DMA(()),
            pltpu.SemaphoreType.DMA(()),
            pltpu.SemaphoreType.DMA(()),
        ],
        compiler_params=pltpu.CompilerParams(vmem_limit_bytes=20 * 2**20),
        cost_estimate=pl.CostEstimate(flops=10**8, bytes_accessed=10**7, transcendentals=0),
    )(*parts, w, tw)


def body(fs, fn, ms, mn, cs, cn, decay, amplitude, fb, mb, cb):
    fs, fn, ms, mn = (a.transpose(0, 2, 1, 3) for a in (fs, fn, ms, mn))
    big = [pltpu.with_memory_space_constraint(a, pltpu.HBM) for a in (fs, fn, ms, mn, fb, mb, cs, cn, cb)]
    parts = spectral_call(*big, decay, amplitude)
    fine_next, medium_next, coarse_next, pattern = synthesis_call(*parts)
    return (fine_next.transpose(0, 2, 1, 3), medium_next.transpose(0, 2, 1, 3), coarse_next, pattern)


def solution(mesh):
    both = ("scale", "lat")
    return jax.shard_map(
        body,
        mesh=mesh,
        in_specs=(
            P(None, None, both, None),
            P(None, None, both, None),
            P(None, None, both, None),
            P(None, None, both, None),
            P("lat", None, None, None),
            P("lat", None, None, None),
            P(),
            P(),
            P(both, None, None),
            P(both, None, None),
            P(both, None, None),
        ),
        out_specs=(
            P(None, None, both, None),
            P(None, None, both, None),
            P("lat", None, None, None),
            P(None, both, None),
        ),
        check_vma=False,
    )
```

```python
import math

import jax
import jax.numpy as jnp
import numpy as np
from jax import lax
from jax.experimental import pallas as pl
from jax.experimental.pallas import tpu as pltpu
from jax.sharding import PartitionSpec as P

LOGICAL = pl.DeviceIdType.LOGICAL
F32, BF16 = jnp.float32, jnp.bfloat16
HBM = pl.BlockSpec(memory_space=pltpu.HBM)
VMEM = pl.BlockSpec(memory_space=pltpu.VMEM)
SMEM = pl.BlockSpec(memory_space=pltpu.SMEM)
MF, MM, MC, NLON, NE, NR = 1280, 640, 160, 2560, 64, 128
ND = 128
NT = (((1,), (1,)), ((), ()))


def my_place():
    return lax.axis_index("scale") * 64 + lax.axis_index("lat")


BLOCKS = [(0, 0), (0, 1), (2, 0), (1, 0), (1, 1)]


def others(me, act):
    @pl.loop(0, 9)
    def _(t):
        for k in range(14):
            d = me + (1 + 9 * k) + t
            act(jnp.where(d >= ND, d - ND, d))

    d = me + (ND - 1)
    act(jnp.where(d >= ND, d - ND, d))


def send_all(me, src, dst, send, recv, here):
    pltpu.make_async_copy(src.at[me], dst.at[me], here).start()

    def one(d):
        pltpu.make_async_remote_copy(
            src.at[d], dst.at[me], send, recv, device_id=d, device_id_type=LOGICAL
        ).start()

    others(me, one)


def wait_rows(ref, count, sem):
    part = ref.at[pl.ds(0, count)]
    pltpu.make_async_copy(part, part, sem).wait()


def spectral_kernel(
    fs, fn, ms, mn, fb, mb, cs, cn, cb, dec, amp,
    s_buf, c_next, r1, r2, rx,
    n_buf, n_flat, fb_buf, mb_buf, a_buf, acc, stage, g1, g2, gx,
    cs_buf, cn_buf, cb_buf, pad, c_stage, c_msg, c_got,
    s_sem, n_sem, b_sem, c_sem, send, recv, here,
):
    me = my_place()
    scale = lax.axis_index("scale")

    coarse_in = (
        pltpu.make_async_copy(cs, cs_buf, c_sem.at[0]),
        pltpu.make_async_copy(cn, cn_buf, c_sem.at[1]),
        pltpu.make_async_copy(cb, cb_buf, c_sem.at[2]),
    )
    for copy in coarse_in:
        copy.start()

    basis = [
        pltpu.make_async_copy(fb.at[pl.ds(0, 5)], fb_buf.at[pl.ds(0, 5)], b_sem.at[0]),
        pltpu.make_async_copy(fb.at[pl.ds(5, 5)], fb_buf.at[pl.ds(5, 5)], b_sem.at[1]),
        pltpu.make_async_copy(mb, mb_buf, b_sem.at[2]),
    ]
    started = set()
    for u, (grp, q) in enumerate(BLOCKS):
        for kt in range(5):
            lanes = pl.ds((q * 5 + kt) * 128, 128)
            rows = s_buf.at[u].reshape(5 * 64, 5, 2, 128).at[pl.ds(kt * 64, 64)]
            if grp == 2:
                src, nsrc, mid = ms, mn, slice(None)
            else:
                src, nsrc, mid = fs, fn, pl.ds(grp * 5, 5)
            pltpu.make_async_copy(src.at[:, mid, :, lanes], rows, s_sem.at[u]).start()
            pltpu.make_async_copy(nsrc.at[:, mid, :, lanes], n_buf.at[u, pl.ds(kt * 64, 64)], n_sem.at[u]).start()
        if grp not in started:
            started.add(grp)
            basis[grp].start()

    barrier = pltpu.get_barrier_semaphore()

    others(me, lambda d: pl.semaphore_signal(barrier, inc=1, device_id=d, device_id_type=LOGICAL))

    for copy in coarse_in:
        copy.wait()
    cdeg = lax.broadcasted_iota(jnp.int32, (MC, MC), 0) + lax.broadcasted_iota(jnp.int32, (MC, MC), 1)
    for c in range(2):
        val = dec[2] * cs_buf[0, c] + amp[2] * cn_buf[0, c].astype(F32)
        c_next[0, c] = jnp.where(cdeg < MC, val, 0.0)
    pad[...] = jnp.zeros_like(pad)
    pad[0, :, pl.ds(0, MC)] = c_next[0, scale]
    pad[1, :, pl.ds(0, MC)] = cb_buf[0].astype(F32)
    for k in range(2):
        c_stage[pl.ds(2 * k, 128, stride=4), :] = pad[k, pl.ds(0, 128), pl.ds(0, 128)]
        extra = jnp.concatenate(
            [pad[k, pl.ds(0, 32), pl.ds(128, 128)], pad[k, pl.ds(128, 32), pl.ds(0, 128)], jnp.zeros((64, 128), F32)], axis=0
        )
        c_stage[pl.ds(2 * k + 1, 128, stride=4), :] = extra
    c_msg.reshape(512, 128)[...] = c_stage[...].astype(BF16)

    rows40 = lax.broadcasted_iota(jnp.int32, (40, 128), 0)
    deg = lax.div(lax.rem(rows40, 10), 2) + lax.broadcasted_iota(jnp.int32, (40, 128), 1)

    def advance(u, kt):
        grp, q = BLOCKS[u]
        which = 1 if grp == 2 else 0
        size = MM if grp == 2 else MF
        first = me * 5 if grp == 2 else me * 10 + grp * 5
        d, a = dec[which], amp[which]
        inside = deg < size - first - (q * 5 + kt) * 128
        inside = jnp.concatenate([inside, inside], axis=0)

        @pl.loop(0, 8)
        def _(j):
            r = pl.ds(pl.multiple_of(kt * 640 + j * 80, 80), 80)
            n_flat[...] = n_buf.at[u].reshape(3200, 128)[r, :]
            val = d * s_buf[u, r, :] + a * n_flat[...].astype(F32)
            s_buf[u, r, :] = jnp.where(inside, val, 0.0)

        for m in range(5):
            for c in range(2):
                v = s_buf[u, pl.ds(kt * 640 + m * 2 + c, 64, stride=10), :]
                a_buf[m, pl.ds(c * 64, 64), pl.ds(kt * 128, 128)] = v.astype(BF16)

    def legendre(u, put):
        grp, q = BLOCKS[u]
        for m in range(5):
            b = mb_buf[m] if grp == 2 else fb_buf[grp * 5 + m, :, pl.ds(q * 640, 640)]
            out = lax.dot_general(b, a_buf[m], NT, preferred_element_type=F32)
            if grp < 2 and q == 0:
                acc[m] = out
            else:
                put(m, out + acc[m] if grp < 2 else out)

    def begin(u):
        pltpu.make_async_copy(s_buf.at[u], s_buf.at[u], s_sem.at[u]).wait()
        pltpu.make_async_copy(n_buf.at[u], n_buf.at[u], n_sem.at[u]).wait()

    def block(u, put, after_first=None):
        begin(u)
        for kt in range(5):
            advance(u, kt)
            if kt == 0 and after_first is not None:
                after_first()
        if BLOCKS[u][1] == 0:
            basis[BLOCKS[u][0]].wait()
        legendre(u, put)

    def put_first(m, out):
        stage[pl.ds(m, 128, stride=10), :] = out

    def put_medium(m, out):
        stage[pl.ds(5 + m, 128, stride=10), :] = out

    block(0, None)
    pl.semaphore_wait(barrier, ND - 1)
    send_all(me, c_msg, c_got, send.at[3], recv.at[3], here.at[3])
    block(1, put_first)
    block(2, put_medium)
    g1.reshape(1280, 128)[...] = stage[...].astype(BF16)
    block(3, None, lambda: send_all(me, g1, r1, send.at[0], recv.at[0], here.at[0]))

    wait_rows(c_got, ND - 1, recv.at[3])
    pltpu.make_async_copy(c_got.at[me], c_got.at[me], here.at[3]).wait()
    c_stage[...] = c_got.reshape(512, 128)[...].astype(F32)
    part = [c_stage[pl.ds(k, 128, stride=4), :].astype(BF16) for k in range(4)]
    main = lax.dot_general(part[2], part[0], NT, preferred_element_type=F32)
    extra = lax.dot_general(part[3], part[1], NT, preferred_element_type=F32)
    stage[pl.ds(5, 128, stride=6), :] = main + jnp.where(me < 32, extra, 0.0)
    c_stage[pl.ds(0, 128, stride=2), :] = extra
    c_stage[pl.ds(1, 128, stride=2), :] = jnp.zeros((128, 128), F32)
    gx.reshape(256, 128)[...] = c_stage[pl.ds(0, 256), :].astype(BF16)
    wide = jnp.logical_and(me >= 32, me < 64)
    slot = lax.rem(me, 32)

    def send_extra():
        @pl.when(wide)
        def _():
            pltpu.make_async_copy(gx.at[me], rx.at[slot], here.at[4]).start()

            def one(d):
                pltpu.make_async_remote_copy(
                    gx.at[d], rx.at[slot], send.at[4], recv.at[4], device_id=d, device_id_type=LOGICAL
                ).start()

            others(me, one)

    def put_last(m, out):
        stage[pl.ds(m, 128, stride=6), :] = out

    block(4, put_last, send_extra)
    g2.reshape(768, 128)[...] = stage[pl.ds(0, 768), :].astype(BF16)
    send_all(me, g2, r2, send.at[1], recv.at[1], here.at[1])

    wait_rows(c_got, ND - 1, send.at[3])

    @pl.when(wide)
    def _():
        pltpu.make_async_copy(gx.at[0], rx.at[0], here.at[4]).wait()
        wait_rows(gx, ND - 1, send.at[4])
        wait_rows(rx, 31, recv.at[4])

    @pl.when(jnp.logical_not(wide))
    def _():
        wait_rows(rx, 32, recv.at[4])

    for k, r in enumerate((r1, r2)):
        pltpu.make_async_copy(r.at[0], r.at[0], here.at[k]).wait()
        wait_rows(r, ND - 1, send.at[k])
        wait_rows(r, ND - 1, recv.at[k])


def spectral_call(fs, fn, ms, mn, fb, mb, cs, cn, cb, dec, amp):
    dma = pltpu.SemaphoreType.DMA
    v = pltpu.VMEM
    return pl.pallas_call(
        spectral_kernel,
        name="spectral",
        out_shape=(
            v((5, 3200, 128), F32),
            v((1, 2, MC, MC), F32),
            v((ND, 5, 2, 128), BF16),
            v((ND, 3, 2, 128), BF16),
            v((32, 2, 128), BF16),
        ),
        in_specs=[HBM] * 9 + [SMEM] * 2,
        out_specs=(VMEM,) * 5,
        scratch_shapes=[
            v((5, 320, 5, 2, 128), BF16),
            v((80, 128), BF16),
            v((10, 128, MF), BF16),
            v((5, 128, MM), BF16),
            v((5, 128, 640), BF16),
            v((5, 128, 128), F32),
            v((1280, 128), F32),
            v((ND, 5, 2, 128), BF16),
            v((ND, 3, 2, 128), BF16),
            v((ND, 2, 128), BF16),
            v((1, 2, MC, MC), F32),
            v((1, 2, MC, MC), BF16),
            v((1, MC, MC), BF16),
            v((2, MC, 256), F32),
            v((512, 128), F32),
            v((ND, 4, 128), BF16),
            v((ND, 4, 128), BF16),
            dma((5,)),
            dma((5,)),
            dma((3,)),
            dma((3,)),
            dma((5,)),
            dma((5,)),
            dma((5,)),
        ],
        compiler_params=pltpu.CompilerParams(has_side_effects=True, collective_id=0, vmem_limit_bytes=30 * 2**20),
        cost_estimate=pl.CostEstimate(flops=10**9, bytes_accessed=25 * 10**6, transcendentals=0),
    )(fs, fn, ms, mn, fb, mb, cs, cn, cb, dec, amp)


def synthesis_kernel(s_buf, c_next, r1, r2, rx, w, tw, fo, mo, co, pat, f1, f2, cf, x, y, pv, o_sem, c_sem, p_sem):
    for u, (grp, q) in enumerate(BLOCKS):
        for kt in range(5):
            rows = s_buf.at[u].reshape(5 * 64, 5, 2, 128).at[pl.ds(kt * 64, 64)]
            dst, mid = (mo, slice(None)) if grp == 2 else (fo, pl.ds(grp * 5, 5))
            pltpu.make_async_copy(rows, dst.at[:, mid, :, pl.ds((q * 5 + kt) * 128, 128)], o_sem).start()
    coarse_out = pltpu.make_async_copy(c_next, co, c_sem)
    coarse_out.start()

    f1[...] = r1.reshape(1280, 128)[...].astype(F32)
    f2[...] = r2.reshape(768, 128)[...].astype(F32)
    cf[pl.ds(0, 128), :] = f2[pl.ds(5, 128, stride=6), :]
    y[pl.ds(0, 64), pl.ds(0, 128)] = rx.reshape(64, 128)[...].astype(F32)
    cf[pl.ds(128, 32), :] = y[pl.ds(0, 64), pl.ds(0, 128)].reshape(32, 2, 128)[:, 0, :]
    for i in range(10):
        if i < 5:
            f = f1[pl.ds(i, 128, stride=10), :]
        else:
            f = f2[pl.ds(i - 5, 128, stride=6), :]
        med = f1[pl.ds(5 + i % 5 + 10 * (i // 5), 64, stride=20), :]
        coarse = cf[pl.ds(i, 16, stride=10), :]
        f = jnp.concatenate([f[:16] + (med[:16] + coarse), f[16:64] + med[16:], f[64:]], axis=0)
        if i == 0:
            row = lax.broadcasted_iota(jnp.int32, (128, 128), 0)
            f = jnp.where(row == 0, f, 2.0 * f)
        else:
            f = 2.0 * f
        t = f.T.astype(BF16)
        x[pl.ds(i * 64, 64), pl.ds(0, 128)] = t[:64]
        x[pl.ds(i * 64, 64), pl.ds(128, 128)] = t[64:]
    y[...] = jnp.dot(x[...], w[...], preferred_element_type=F32)
    view = pv.reshape(20 * 64, 1, 128)
    for half in range(2):
        for j in range(5):
            col = pl.ds(j * 256 + half * 128, 128)
            parts = [None, None]
            for i in range(10):
                yr = y[pl.ds(i * 64, 64), pl.ds(half * 128, 128)]
                if i == 0:
                    term = yr
                else:
                    yi = y[pl.ds(i * 64, 64), pl.ds(256 + half * 128, 128)]
                    term = tw[pl.ds(i, 1), col] * yr - tw[pl.ds(16 + i, 1), col] * yi
                k = i % 2
                parts[k] = term if parts[k] is None else parts[k] + term
            for k, val in ((0, parts[0] + parts[1]), (5, parts[0] - parts[1])):
                lt = (j + k) * 2 + half
                pv[pl.ds(lt * 64, 64), :] = jnp.tanh(val)
                pltpu.make_async_copy(view.at[pl.ds(lt * 64, 64)], pat.at[:, :, pl.ds(lt * 128, 128)], p_sem).start()
    pltpu.make_async_copy(s_buf, s_buf, o_sem).wait()
    coarse_out.wait()
    pltpu.make_async_copy(pv, pv, p_sem).wait()


def synthesis_call(*parts):
    p = np.arange(128)[:, None]
    ang = 2.0 * math.pi * ((p * np.arange(256)[None, :]) % 256) / 256.0
    c, s = np.cos(ang), np.sin(ang)
    w = jnp.asarray(np.block([[c, s], [-s, c]]), BF16)
    i = np.arange(16)[:, None]
    ang = 2.0 * math.pi * ((i * np.arange(1280)[None, :]) % NLON) / NLON
    tw = jnp.asarray(np.concatenate([np.cos(ang), np.sin(ang)]), F32)
    s = jax.ShapeDtypeStruct
    v = pltpu.VMEM
    return pl.pallas_call(
        synthesis_kernel,
        name="synthesis",
        out_shape=(
            s((NE, 10, 2, MF), F32),
            s((NE, 5, 2, MM), F32),
            s((1, 2, MC, MC), F32),
            s((NE, 1, NLON), F32),
        ),
        in_specs=[VMEM] * 7,
        out_specs=(HBM,) * 4,
        scratch_shapes=[
            v((1280, 128), F32),
            v((768, 128), F32),
            v((160, 128), F32),
            v((640, 256), BF16),
            v((640, 512), F32),
            v((1280, 128), F32),
            pltpu.SemaphoreType.DMA(()),
            pltpu.SemaphoreType.DMA(()),
            pltpu.SemaphoreType.DMA(()),
        ],
        compiler_params=pltpu.CompilerParams(vmem_limit_bytes=20 * 2**20),
        cost_estimate=pl.CostEstimate(flops=10**8, bytes_accessed=10**7, transcendentals=0),
    )(*parts, w, tw)


def body(fs, fn, ms, mn, cs, cn, decay, amplitude, fb, mb, cb):
    fs, fn, ms, mn = (a.transpose(0, 2, 1, 3) for a in (fs, fn, ms, mn))
    big = [pltpu.with_memory_space_constraint(a, pltpu.HBM) for a in (fs, fn, ms, mn, fb, mb, cs, cn, cb)]
    parts = spectral_call(*big, decay, amplitude)
    fine_next, medium_next, coarse_next, pattern = synthesis_call(*parts)
    return (fine_next.transpose(0, 2, 1, 3), medium_next.transpose(0, 2, 1, 3), coarse_next, pattern)


def solution(mesh):
    both = ("scale", "lat")
    return jax.shard_map(
        body,
        mesh=mesh,
        in_specs=(
            P(None, None, both, None),
            P(None, None, both, None),
            P(None, None, both, None),
            P(None, None, both, None),
            P("lat", None, None, None),
            P("lat", None, None, None),
            P(),
            P(),
            P(both, None, None),
            P(both, None, None),
            P(both, None, None),
        ),
        out_specs=(
            P(None, None, both, None),
            P(None, None, both, None),
            P("lat", None, None, None),
            P(None, both, None),
        ),
        check_vma=False,
    )
```

```python
import math

import jax
import jax.numpy as jnp
import numpy as np
from jax import lax
from jax.experimental import pallas as pl
from jax.experimental.pallas import tpu as pltpu
from jax.sharding import PartitionSpec as P

LOGICAL = pl.DeviceIdType.LOGICAL
F32, BF16 = jnp.float32, jnp.bfloat16
HBM = pl.BlockSpec(memory_space=pltpu.HBM)
VMEM = pl.BlockSpec(memory_space=pltpu.VMEM)
MF, MM, MC, NLON, NE, NR = 1280, 640, 160, 2560, 64, 128
ND = 128
NT = (((1,), (1,)), ((), ()))


def my_place():
    return lax.axis_index("scale") * 64 + lax.axis_index("lat")


BLOCKS = [(2, 0), (0, 0), (0, 1), (1, 0), (1, 1)]


def others(act):
    lat = lax.axis_index("lat")
    y = lax.axis_index("scale") * 2 + lax.rem(lax.div(lat, 2), 2)
    x, z, core = lax.div(lat, 16), lax.rem(lax.div(lat, 4), 4), lax.rem(lat, 2)
    low = []
    for dy in (2, 1, 3, 0):
        for dc in (1, 0):
            yy = lax.rem(y + dy, 4)
            low.append(lax.div(yy, 2) * 64 + lax.rem(yy, 2) * 2 + lax.rem(core + dc, 2))

    @pl.loop(0, 15)
    def _(t):
        high = lax.rem(x + 1 + lax.div(t, 4), 4) * 16 + lax.rem(z + 1 + t, 4) * 4
        for part in low:
            act(high + part)

    for part in low[:-1]:
        act(x * 16 + z * 4 + part)


def send_all(me, src, dst, send, recv, here):
    pltpu.make_async_copy(src.at[me], dst.at[me], here).start()

    def one(d):
        pltpu.make_async_remote_copy(
            src.at[d], dst.at[me], send, recv, device_id=d, device_id_type=LOGICAL
        ).start()

    others(one)


def wait_rows(ref, count, sem):
    part = ref.at[pl.ds(0, count)]
    pltpu.make_async_copy(part, part, sem).wait()


def spectral_kernel(
    fs, fn, ms, mn, fb, mb, cs, cn, cb, dec_in, amp_in,
    s_buf, c_next, r1, r2, r3, rc,
    n_buf, n_flat, fb_buf, mb_buf, a_buf, acc, stage1, stage2, stage3, g1, g2, g3, gc,
    cs_buf, cn_buf, cb_buf, pad, c_stage, c_msg, c_got,
    dec, amp, s_sem, n_sem, b_sem, c_sem, send, recv, here,
):
    me = my_place()
    scale = lax.axis_index("scale")

    coarse_in = (
        pltpu.make_async_copy(cs, cs_buf, c_sem.at[0]),
        pltpu.make_async_copy(cn, cn_buf, c_sem.at[1]),
        pltpu.make_async_copy(cb, cb_buf, c_sem.at[2]),
        pltpu.make_async_copy(dec_in, dec, c_sem.at[3]),
        pltpu.make_async_copy(amp_in, amp, c_sem.at[4]),
    )
    for copy in coarse_in:
        copy.start()

    barrier = pltpu.get_barrier_semaphore()

    others(lambda d: pl.semaphore_signal(barrier, inc=1, device_id=d, device_id_type=LOGICAL))

    basis = [
        pltpu.make_async_copy(fb.at[pl.ds(0, 5)], fb_buf.at[pl.ds(0, 5)], b_sem.at[0]),
        pltpu.make_async_copy(fb.at[pl.ds(5, 5)], fb_buf.at[pl.ds(5, 5)], b_sem.at[1]),
        pltpu.make_async_copy(mb, mb_buf, b_sem.at[2]),
    ]
    started = set()
    for u, (grp, q) in enumerate(BLOCKS):
        for kt in range(5):
            lanes = pl.ds((q * 5 + kt) * 128, 128)
            rows = s_buf.at[u].reshape(5 * 64, 5, 2, 128).at[pl.ds(kt * 64, 64)]
            if grp == 2:
                src, nsrc, mid = ms, mn, slice(None)
            else:
                src, nsrc, mid = fs, fn, pl.ds(grp * 5, 5)
            pltpu.make_async_copy(src.at[:, mid, :, lanes], rows, s_sem.at[u]).start()
            pltpu.make_async_copy(nsrc.at[:, mid, :, lanes], n_buf.at[u, pl.ds(kt * 64, 64)], n_sem.at[u]).start()
        if grp not in started:
            started.add(grp)
            basis[grp].start()

    for copy in coarse_in:
        copy.wait()
    cdeg = lax.broadcasted_iota(jnp.int32, (MC, MC), 0) + lax.broadcasted_iota(jnp.int32, (MC, MC), 1)
    for c in range(2):
        val = dec[2] * cs_buf[0, c] + amp[2] * cn_buf[0, c].astype(F32)
        c_next[0, c] = jnp.where(cdeg < MC, val, 0.0)
    pad[...] = jnp.zeros_like(pad)
    pad[0, :, pl.ds(0, MC)] = c_next[0, scale]
    pad[1, :, pl.ds(0, MC)] = cb_buf[0].astype(F32)
    for k in range(2):
        c_stage[pl.ds(2 * k, 128, stride=4), :] = pad[k, pl.ds(0, 128), pl.ds(0, 128)]
        extra = jnp.concatenate(
            [pad[k, pl.ds(0, 32), pl.ds(128, 128)], pad[k, pl.ds(128, 32), pl.ds(0, 128)], jnp.zeros((64, 128), F32)], axis=0
        )
        c_stage[pl.ds(2 * k + 1, 128, stride=4), :] = extra
    c_msg.reshape(512, 128)[...] = c_stage[...].astype(BF16)

    rows40 = lax.broadcasted_iota(jnp.int32, (40, 128), 0)
    deg = lax.div(lax.rem(rows40, 10), 2) + lax.broadcasted_iota(jnp.int32, (40, 128), 1)

    def advance(u, kt):
        grp, q = BLOCKS[u]
        which = 1 if grp == 2 else 0
        size = MM if grp == 2 else MF
        first = me * 5 if grp == 2 else me * 10 + grp * 5
        d, a = dec[which], amp[which]
        inside = deg < size - first - (q * 5 + kt) * 128
        inside = jnp.concatenate([inside, inside], axis=0)
        noise = n_buf.at[u].reshape(3200, 128)
        for j in range(8):
            r = pl.ds(kt * 640 + j * 80, 80)
            n_flat[pl.ds(j * 80, 80), :] = noise[r, :]
            val = d * s_buf[u, r, :] + a * n_flat[pl.ds(j * 80, 80), :].astype(F32)
            s_buf[u, r, :] = jnp.where(inside, val, 0.0)
        for m in range(5):
            for c in range(2):
                v = s_buf[u, pl.ds(kt * 640 + m * 2 + c, 64, stride=10), :]
                a_buf[u % 2, m, pl.ds(c * 64, 64), pl.ds(kt * 128, 128)] = v.astype(BF16)

    def legendre(u, m):
        grp, q = BLOCKS[u]
        b = mb_buf[m] if grp == 2 else fb_buf[grp * 5 + m, :, pl.ds(q * 640, 640)]
        out = lax.dot_general(b, a_buf[u % 2, m], NT, preferred_element_type=F32)
        if grp < 2 and q == 0:
            acc[m] = out
        else:
            put[u](m, out + acc[m] if grp < 2 else out)

    def run(u, store=None, post=None):
        if u < 5:
            pltpu.make_async_copy(s_buf.at[u], s_buf.at[u], s_sem.at[u]).wait()
            pltpu.make_async_copy(n_buf.at[u], n_buf.at[u], n_sem.at[u]).wait()
        if u > 0 and BLOCKS[u - 1][1] == 0:
            basis[BLOCKS[u - 1][0]].wait()
        for k in range(5):
            if u > 0:
                for m in ((0, 1), (2, 3), (4,), (), ())[k]:
                    legendre(u - 1, m)
            if u < 5:
                advance(u, k)
            if k == 2 and store is not None:
                store()
            if k == 3 and post is not None:
                post()

    def put_medium(m, out):
        stage1[pl.ds(m, 128, stride=6), :] = out

    def put_first(m, out):
        if m < 4:
            stage2[pl.ds(m, 128, stride=4), :] = out
        else:
            stage3[pl.ds(0, 128, stride=6), :] = out

    def put_last(m, out):
        stage3[pl.ds(1 + m, 128, stride=6), :] = out

    def store1():
        g1.reshape(768, 128)[...] = stage1[...].astype(BF16)

    def store2():
        g2.reshape(512, 128)[...] = stage2[...].astype(BF16)

    put = {0: put_medium, 2: put_first, 4: put_last}
    stage1[pl.ds(5, 128, stride=6), :] = jnp.zeros((128, 128), F32)
    run(0)
    pl.semaphore_wait(barrier, ND - 1)
    send_all(me, c_msg, c_got, send.at[3], recv.at[3], here.at[3])
    run(1, store1, lambda: send_all(me, g1, r1, send.at[0], recv.at[0], here.at[0]))
    run(2)
    run(3, store2, lambda: send_all(me, g2, r2, send.at[1], recv.at[1], here.at[1]))
    run(4)
    run(5)
    g3.reshape(768, 128)[...] = stage3[...].astype(BF16)
    send_all(me, g3, r3, send.at[2], recv.at[2], here.at[2])

    wait_rows(c_got, ND - 1, recv.at[3])
    pltpu.make_async_copy(c_got.at[me], c_got.at[me], here.at[3]).wait()
    c_stage[...] = c_got.reshape(512, 128)[...].astype(F32)
    part = [c_stage[pl.ds(k, 128, stride=4), :].astype(BF16) for k in range(4)]
    main = lax.dot_general(part[2], part[0], NT, preferred_element_type=F32)
    extra = lax.dot_general(part[3], part[1], NT, preferred_element_type=F32)
    c_stage[pl.ds(0, 128, stride=2), :] = main + jnp.where(me < 32, extra, 0.0)
    c_stage[pl.ds(1, 128, stride=2), :] = extra
    gc.reshape(256, 128)[...] = c_stage[pl.ds(0, 256), :].astype(BF16)
    send_all(me, gc, rc, send.at[4], recv.at[4], here.at[4])

    wait_rows(c_got, ND - 1, send.at[3])
    for k, r in enumerate((r1, r2, r3)):
        pltpu.make_async_copy(r.at[0], r.at[0], here.at[k]).wait()
        wait_rows(r, ND - 1, send.at[k])
        wait_rows(r, ND - 1, recv.at[k])
    pltpu.make_async_copy(rc.at[0], rc.at[0], here.at[4]).wait()
    wait_rows(rc, ND - 1, send.at[4])
    wait_rows(rc, ND - 1, recv.at[4])


def spectral_call(fs, fn, ms, mn, fb, mb, cs, cn, cb, dec, amp):
    dma = pltpu.SemaphoreType.DMA
    v = pltpu.VMEM
    return pl.pallas_call(
        spectral_kernel,
        name="spectral",
        out_shape=(
            v((5, 3200, 128), F32),
            v((1, 2, MC, MC), F32),
            v((ND, 3, 2, 128), BF16),
            v((ND, 2, 2, 128), BF16),
            v((ND, 3, 2, 128), BF16),
            v((ND, 2, 128), BF16),
        ),
        in_specs=[HBM] * 11,
        out_specs=(VMEM,) * 6,
        scratch_shapes=[
            v((5, 320, 5, 2, 128), BF16),
            v((640, 128), BF16),
            v((10, 128, MF), BF16),
            v((5, 128, MM), BF16),
            v((2, 5, 128, 640), BF16),
            v((5, 128, 128), F32),
            v((768, 128), F32),
            v((512, 128), F32),
            v((768, 128), F32),
            v((ND, 3, 2, 128), BF16),
            v((ND, 2, 2, 128), BF16),
            v((ND, 3, 2, 128), BF16),
            v((ND, 2, 128), BF16),
            v((1, 2, MC, MC), F32),
            v((1, 2, MC, MC), BF16),
            v((1, MC, MC), BF16),
            v((2, MC, 256), F32),
            v((512, 128), F32),
            v((ND, 4, 128), BF16),
            v((ND, 4, 128), BF16),
            pltpu.SMEM((3,), F32),
            pltpu.SMEM((3,), F32),
            dma((5,)),
            dma((5,)),
            dma((3,)),
            dma((5,)),
            dma((5,)),
            dma((5,)),
            dma((5,)),
        ],
        compiler_params=pltpu.CompilerParams(has_side_effects=True, collective_id=0, vmem_limit_bytes=30 * 2**20),
        cost_estimate=pl.CostEstimate(flops=10**9, bytes_accessed=25 * 10**6, transcendentals=0),
    )(fs, fn, ms, mn, fb, mb, cs, cn, cb, dec, amp)


def synthesis_kernel(s_buf, c_next, r1, r2, r3, rc, w, tw, fo, mo, co, pat, f1, f2, f3, fc, cf, x, y, pv, o_sem, c_sem, p_sem):
    for u, (grp, q) in enumerate(BLOCKS):
        for kt in range(5):
            rows = s_buf.at[u].reshape(5 * 64, 5, 2, 128).at[pl.ds(kt * 64, 64)]
            dst, mid = (mo, slice(None)) if grp == 2 else (fo, pl.ds(grp * 5, 5))
            pltpu.make_async_copy(rows, dst.at[:, mid, :, pl.ds((q * 5 + kt) * 128, 128)], o_sem).start()
    coarse_out = pltpu.make_async_copy(c_next, co, c_sem)
    coarse_out.start()

    f1[...] = r1.reshape(768, 128)[...].astype(F32)
    f2[...] = r2.reshape(512, 128)[...].astype(F32)
    f3[...] = r3.reshape(768, 128)[...].astype(F32)
    fc[...] = rc.reshape(256, 128)[...].astype(F32)
    cf[pl.ds(0, 128), :] = fc[pl.ds(0, 128, stride=2), :]
    cf[pl.ds(128, 32), :] = fc[pl.ds(65, 32, stride=2), :]
    for i in range(10):
        if i < 4:
            f = f2[pl.ds(i, 128, stride=4), :]
        else:
            f = f3[pl.ds(i - 4, 128, stride=6), :]
        med = f1[pl.ds(i % 5 + 6 * (i // 5), 64, stride=12), :]
        coarse = cf[pl.ds(i, 16, stride=10), :]
        f = jnp.concatenate([f[:16] + (med[:16] + coarse), f[16:64] + med[16:], f[64:]], axis=0)
        if i == 0:
            row = lax.broadcasted_iota(jnp.int32, (128, 128), 0)
            f = jnp.where(row == 0, f, 2.0 * f)
        else:
            f = 2.0 * f
        t = f.T.astype(BF16)
        x[pl.ds(i * 64, 64), pl.ds(0, 128)] = t[:64]
        x[pl.ds(i * 64, 64), pl.ds(128, 128)] = t[64:]
    y[...] = jnp.dot(x[...], w[...], preferred_element_type=F32)
    view = pv.reshape(20 * 64, 1, 128)
    for half in range(2):
        for j in range(5):
            col = pl.ds(j * 256 + half * 128, 128)
            parts = [None, None]
            for i in range(10):
                yr = y[pl.ds(i * 64, 64), pl.ds(half * 128, 128)]
                if i == 0:
                    term = yr
                else:
                    yi = y[pl.ds(i * 64, 64), pl.ds(256 + half * 128, 128)]
                    term = tw[pl.ds(i, 1), col] * yr - tw[pl.ds(16 + i, 1), col] * yi
                k = i % 2
                parts[k] = term if parts[k] is None else parts[k] + term
            for k, val in ((0, parts[0] + parts[1]), (5, parts[0] - parts[1])):
                lt = (j + k) * 2 + half
                pv[pl.ds(lt * 64, 64), :] = jnp.tanh(val)
                pltpu.make_async_copy(view.at[pl.ds(lt * 64, 64)], pat.at[:, :, pl.ds(lt * 128, 128)], p_sem).start()
    pltpu.make_async_copy(s_buf, s_buf, o_sem).wait()
    coarse_out.wait()
    pltpu.make_async_copy(pv, pv, p_sem).wait()


def synthesis_call(*parts):
    p = np.arange(128)[:, None]
    ang = 2.0 * math.pi * ((p * np.arange(256)[None, :]) % 256) / 256.0
    c, s = np.cos(ang), np.sin(ang)
    w = jnp.asarray(np.block([[c, s], [-s, c]]), BF16)
    i = np.arange(16)[:, None]
    ang = 2.0 * math.pi * ((i * np.arange(1280)[None, :]) % NLON) / NLON
    tw = jnp.asarray(np.concatenate([np.cos(ang), np.sin(ang)]), F32)
    s = jax.ShapeDtypeStruct
    v = pltpu.VMEM
    return pl.pallas_call(
        synthesis_kernel,
        name="synthesis",
        out_shape=(
            s((NE, 10, 2, MF), F32),
            s((NE, 5, 2, MM), F32),
            s((1, 2, MC, MC), F32),
            s((NE, 1, NLON), F32),
        ),
        in_specs=[VMEM] * 8,
        out_specs=(HBM,) * 4,
        scratch_shapes=[
            v((768, 128), F32),
            v((512, 128), F32),
            v((768, 128), F32),
            v((256, 128), F32),
            v((160, 128), F32),
            v((640, 256), BF16),
            v((640, 512), F32),
            v((1280, 128), F32),
            pltpu.SemaphoreType.DMA(()),
            pltpu.SemaphoreType.DMA(()),
            pltpu.SemaphoreType.DMA(()),
        ],
        compiler_params=pltpu.CompilerParams(vmem_limit_bytes=20 * 2**20),
        cost_estimate=pl.CostEstimate(flops=10**8, bytes_accessed=10**7, transcendentals=0),
    )(*parts, w, tw)


def body(fs, fn, ms, mn, cs, cn, decay, amplitude, fb, mb, cb):
    fs, fn, ms, mn = (a.transpose(0, 2, 1, 3) for a in (fs, fn, ms, mn))
    big = [pltpu.with_memory_space_constraint(a, pltpu.HBM) for a in (fs, fn, ms, mn, fb, mb, cs, cn, cb, decay, amplitude)]
    parts = spectral_call(*big)
    fine_next, medium_next, coarse_next, pattern = synthesis_call(*parts)
    return (fine_next.transpose(0, 2, 1, 3), medium_next.transpose(0, 2, 1, 3), coarse_next, pattern)


def solution(mesh):
    both = ("scale", "lat")
    return jax.shard_map(
        body,
        mesh=mesh,
        in_specs=(
            P(None, None, both, None),
            P(None, None, both, None),
            P(None, None, both, None),
            P(None, None, both, None),
            P("lat", None, None, None),
            P("lat", None, None, None),
            P(),
            P(),
            P(both, None, None),
            P(both, None, None),
            P(both, None, None),
        ),
        out_specs=(
            P(None, None, both, None),
            P(None, None, both, None),
            P("lat", None, None, None),
            P(None, both, None),
        ),
        check_vma=False,
    )
```

```python
import math

import jax
import jax.numpy as jnp
import numpy as np
from jax import lax
from jax.experimental import pallas as pl
from jax.experimental.pallas import tpu as pltpu
from jax.sharding import PartitionSpec as P

LOGICAL = pl.DeviceIdType.LOGICAL
F32, BF16 = jnp.float32, jnp.bfloat16
HBM = pl.BlockSpec(memory_space=pltpu.HBM)
VMEM = pl.BlockSpec(memory_space=pltpu.VMEM)
MF, MM, MC, NLON, NE, NR = 1280, 640, 160, 2560, 64, 128
ND = 128
NT = (((1,), (1,)), ((), ()))


def my_place():
    return lax.axis_index("scale") * 64 + lax.axis_index("lat")


BLOCKS = [(2, 0), (0, 0), (0, 1), (1, 0), (1, 1)]


def targets():
    lat = lax.axis_index("lat")
    y = lax.axis_index("scale") * 2 + lax.rem(lax.div(lat, 2), 2)
    x, z, core = lax.div(lat, 16), lax.rem(lax.div(lat, 4), 4), lax.rem(lat, 2)
    low = []
    for dy in (2, 1, 3, 0):
        for dc in (1, 0):
            yy = lax.rem(y + dy, 4)
            low.append(lax.div(yy, 2) * 64 + lax.rem(yy, 2) * 2 + lax.rem(core + dc, 2))
    return x, z, low


def others(act):
    x, z, low = targets()
    for dx in (2, 1, 3, 0):
        xx = lax.rem(x + dx, 4) * 16

        @pl.loop(1, 5 if dx else 4)
        def _(t):
            high = xx + lax.rem(z + t, 4) * 4
            for part in low:
                act(high + part)

    for part in low[:-1]:
        act(x * 16 + z * 4 + part)


def some_others(act, k):
    x, z, low = targets()
    pairs = [(dx, dz) for dx in (2, 1, 3, 0) for dz in (2, 1, 3, 0)]
    for dx, dz in pairs[3 * k : 3 * k + 3 if k < 4 else 16]:
        high = lax.rem(x + dx, 4) * 16 + lax.rem(z + dz, 4) * 4
        for part in low if dx or dz else low[:-1]:
            act(high + part)


def send_all(me, src, dst, send, recv, here, k=None):
    def one(d):
        pltpu.make_async_remote_copy(
            src.at[d], dst.at[me], send, recv, device_id=d, device_id_type=LOGICAL
        ).start()

    if k is None or k == 0:
        pltpu.make_async_copy(src.at[me], dst.at[me], here).start()
    if k is None:
        others(one)
    else:
        some_others(one, k)


def wait_rows(ref, count, sem):
    part = ref.at[pl.ds(0, count)]
    pltpu.make_async_copy(part, part, sem).wait()


def spectral_kernel(
    fs, fn, ms, mn, fb, mb, cs, cn, cb, dec_in, amp_in,
    s_buf, c_next, r1, r2, r3, rc,
    n_buf, n_flat, fb_buf, mb_buf, a_buf, acc, stage1, stage2, stage3, g1, g2, g3, gc,
    cs_buf, cn_buf, cb_buf, pad, c_stage, c_msg, c_got,
    dec, amp, s_sem, n_sem, b_sem, c_sem, send, recv, here,
):
    me = my_place()
    scale = lax.axis_index("scale")

    coarse_in = (
        pltpu.make_async_copy(cs, cs_buf, c_sem.at[0]),
        pltpu.make_async_copy(cn, cn_buf, c_sem.at[1]),
        pltpu.make_async_copy(cb, cb_buf, c_sem.at[2]),
        pltpu.make_async_copy(dec_in, dec, c_sem.at[3]),
        pltpu.make_async_copy(amp_in, amp, c_sem.at[4]),
    )
    for copy in coarse_in:
        copy.start()

    barrier = pltpu.get_barrier_semaphore()

    others(lambda d: pl.semaphore_signal(barrier, inc=1, device_id=d, device_id_type=LOGICAL))

    basis = [
        pltpu.make_async_copy(fb.at[pl.ds(0, 5)], fb_buf.at[pl.ds(0, 5)], b_sem.at[0]),
        pltpu.make_async_copy(fb.at[pl.ds(5, 5)], fb_buf.at[pl.ds(5, 5)], b_sem.at[1]),
        pltpu.make_async_copy(mb, mb_buf, b_sem.at[2]),
    ]
    started = set()
    for u, (grp, q) in enumerate(BLOCKS):
        for kt in range(5):
            lanes = pl.ds((q * 5 + kt) * 128, 128)
            rows = s_buf.at[u].reshape(5 * 64, 5, 2, 128).at[pl.ds(kt * 64, 64)]
            if grp == 2:
                src, nsrc, mid = ms, mn, slice(None)
            else:
                src, nsrc, mid = fs, fn, pl.ds(grp * 5, 5)
            pltpu.make_async_copy(src.at[:, mid, :, lanes], rows, s_sem.at[u]).start()
            pltpu.make_async_copy(nsrc.at[:, mid, :, lanes], n_buf.at[u, pl.ds(kt * 64, 64)], n_sem.at[u]).start()
        if grp not in started:
            started.add(grp)
            basis[grp].start()

    for copy in coarse_in:
        copy.wait()
    cdeg = lax.broadcasted_iota(jnp.int32, (MC, MC), 0) + lax.broadcasted_iota(jnp.int32, (MC, MC), 1)
    for c in range(2):
        val = dec[2] * cs_buf[0, c] + amp[2] * cn_buf[0, c].astype(F32)
        c_next[0, c] = jnp.where(cdeg < MC, val, 0.0)
    pad[...] = jnp.zeros_like(pad)
    pad[0, :, pl.ds(0, MC)] = c_next[0, scale]
    pad[1, :, pl.ds(0, MC)] = cb_buf[0].astype(F32)
    for k in range(2):
        c_stage[pl.ds(2 * k, 128, stride=4), :] = pad[k, pl.ds(0, 128), pl.ds(0, 128)]
        extra = jnp.concatenate(
            [pad[k, pl.ds(0, 32), pl.ds(128, 128)], pad[k, pl.ds(128, 32), pl.ds(0, 128)], jnp.zeros((64, 128), F32)], axis=0
        )
        c_stage[pl.ds(2 * k + 1, 128, stride=4), :] = extra
    c_msg.reshape(512, 128)[...] = c_stage[...].astype(BF16)

    rows40 = lax.broadcasted_iota(jnp.int32, (40, 128), 0)
    deg = lax.div(lax.rem(rows40, 10), 2) + lax.broadcasted_iota(jnp.int32, (40, 128), 1)

    def advance(u, kt):
        grp, q = BLOCKS[u]
        which = 1 if grp == 2 else 0
        size = MM if grp == 2 else MF
        first = me * 5 if grp == 2 else me * 10 + grp * 5
        d, a = dec[which], amp[which]
        inside = deg < size - first - (q * 5 + kt) * 128
        inside = jnp.concatenate([inside, inside], axis=0)
        noise = n_buf.at[u].reshape(3200, 128)
        for j in range(8):
            r = pl.ds(kt * 640 + j * 80, 80)
            n_flat[pl.ds(j * 80, 80), :] = noise[r, :]
            val = d * s_buf[u, r, :] + a * n_flat[pl.ds(j * 80, 80), :].astype(F32)
            s_buf[u, r, :] = jnp.where(inside, val, 0.0)
        for m in range(5):
            for c in range(2):
                v = s_buf[u, pl.ds(kt * 640 + m * 2 + c, 64, stride=10), :]
                a_buf[u % 2, m, pl.ds(c * 64, 64), pl.ds(kt * 128, 128)] = v.astype(BF16)

    def legendre(u, m):
        grp, q = BLOCKS[u]
        b = mb_buf[m] if grp == 2 else fb_buf[grp * 5 + m, :, pl.ds(q * 640, 640)]
        out = lax.dot_general(b, a_buf[u % 2, m], NT, preferred_element_type=F32)
        if grp < 2 and q == 0:
            acc[m] = out
        else:
            put[u](m, out + acc[m] if grp < 2 else out)

    def run(u, store=None, sends=None):
        if u < 5:
            pltpu.make_async_copy(s_buf.at[u], s_buf.at[u], s_sem.at[u]).wait()
            pltpu.make_async_copy(n_buf.at[u], n_buf.at[u], n_sem.at[u]).wait()
        if u > 0 and BLOCKS[u - 1][1] == 0:
            basis[BLOCKS[u - 1][0]].wait()
        for k in range(5):
            if sends is not None:
                sends(k)
            if u > 0:
                for m in ((0, 1), (2, 3), (4,), (), ())[k]:
                    legendre(u - 1, m)
            if u < 5:
                advance(u, k)
            if k == 2 and store is not None:
                store()

    def put_medium(m, out):
        stage1[pl.ds(m, 128, stride=6), :] = out

    def put_first(m, out):
        if m < 4:
            stage2[pl.ds(m, 128, stride=4), :] = out
        else:
            stage3[pl.ds(0, 128, stride=6), :] = out

    def put_last(m, out):
        stage3[pl.ds(1 + m, 128, stride=6), :] = out

    def store1():
        g1.reshape(768, 128)[...] = stage1[...].astype(BF16)

    def store2():
        g2.reshape(512, 128)[...] = stage2[...].astype(BF16)

    put = {0: put_medium, 2: put_first, 4: put_last}
    stage1[pl.ds(5, 128, stride=6), :] = jnp.zeros((128, 128), F32)
    run(0)
    run(1, store1)
    pl.semaphore_wait(barrier, ND - 1)
    send_all(me, c_msg, c_got, send.at[3], recv.at[3], here.at[3])
    run(2, None, lambda k: send_all(me, g1, r1, send.at[0], recv.at[0], here.at[0], k))
    run(3, store2)
    run(4, None, lambda k: send_all(me, g2, r2, send.at[1], recv.at[1], here.at[1], k))
    run(5)
    g3.reshape(768, 128)[...] = stage3[...].astype(BF16)
    send_all(me, g3, r3, send.at[2], recv.at[2], here.at[2])

    wait_rows(c_got, ND - 1, recv.at[3])
    pltpu.make_async_copy(c_got.at[me], c_got.at[me], here.at[3]).wait()
    c_stage[...] = c_got.reshape(512, 128)[...].astype(F32)
    part = [c_stage[pl.ds(k, 128, stride=4), :].astype(BF16) for k in range(4)]
    main = lax.dot_general(part[2], part[0], NT, preferred_element_type=F32)
    extra = lax.dot_general(part[3], part[1], NT, preferred_element_type=F32)
    c_stage[pl.ds(0, 128, stride=2), :] = main + jnp.where(me < 32, extra, 0.0)
    c_stage[pl.ds(1, 128, stride=2), :] = extra
    gc.reshape(256, 128)[...] = c_stage[pl.ds(0, 256), :].astype(BF16)
    send_all(me, gc, rc, send.at[4], recv.at[4], here.at[4])

    wait_rows(c_got, ND - 1, send.at[3])
    for k, r in enumerate((r1, r2, r3)):
        pltpu.make_async_copy(r.at[0], r.at[0], here.at[k]).wait()
        wait_rows(r, ND - 1, send.at[k])
        wait_rows(r, ND - 1, recv.at[k])
    pltpu.make_async_copy(rc.at[0], rc.at[0], here.at[4]).wait()
    wait_rows(rc, ND - 1, send.at[4])
    wait_rows(rc, ND - 1, recv.at[4])


def spectral_call(fs, fn, ms, mn, fb, mb, cs, cn, cb, dec, amp):
    dma = pltpu.SemaphoreType.DMA
    v = pltpu.VMEM
    return pl.pallas_call(
        spectral_kernel,
        name="spectral",
        out_shape=(
            v((5, 3200, 128), F32),
            v((1, 2, MC, MC), F32),
            v((ND, 3, 2, 128), BF16),
            v((ND, 2, 2, 128), BF16),
            v((ND, 3, 2, 128), BF16),
            v((ND, 2, 128), BF16),
        ),
        in_specs=[HBM] * 11,
        out_specs=(VMEM,) * 6,
        scratch_shapes=[
            v((5, 320, 5, 2, 128), BF16),
            v((640, 128), BF16),
            v((10, 128, MF), BF16),
            v((5, 128, MM), BF16),
            v((2, 5, 128, 640), BF16),
            v((5, 128, 128), F32),
            v((768, 128), F32),
            v((512, 128), F32),
            v((768, 128), F32),
            v((ND, 3, 2, 128), BF16),
            v((ND, 2, 2, 128), BF16),
            v((ND, 3, 2, 128), BF16),
            v((ND, 2, 128), BF16),
            v((1, 2, MC, MC), F32),
            v((1, 2, MC, MC), BF16),
            v((1, MC, MC), BF16),
            v((2, MC, 256), F32),
            v((512, 128), F32),
            v((ND, 4, 128), BF16),
            v((ND, 4, 128), BF16),
            pltpu.SMEM((3,), F32),
            pltpu.SMEM((3,), F32),
            dma((5,)),
            dma((5,)),
            dma((3,)),
            dma((5,)),
            dma((5,)),
            dma((5,)),
            dma((5,)),
        ],
        compiler_params=pltpu.CompilerParams(has_side_effects=True, collective_id=0, vmem_limit_bytes=30 * 2**20),
        cost_estimate=pl.CostEstimate(flops=10**9, bytes_accessed=25 * 10**6, transcendentals=0),
    )(fs, fn, ms, mn, fb, mb, cs, cn, cb, dec, amp)


def synthesis_kernel(s_buf, c_next, r1, r2, r3, rc, w, tw, fo, mo, co, pat, f1, f2, f3, fc, cf, x, y, pv, o_sem, c_sem, p_sem):
    for u, (grp, q) in enumerate(BLOCKS):
        for kt in range(5):
            rows = s_buf.at[u].reshape(5 * 64, 5, 2, 128).at[pl.ds(kt * 64, 64)]
            dst, mid = (mo, slice(None)) if grp == 2 else (fo, pl.ds(grp * 5, 5))
            pltpu.make_async_copy(rows, dst.at[:, mid, :, pl.ds((q * 5 + kt) * 128, 128)], o_sem).start()
    coarse_out = pltpu.make_async_copy(c_next, co, c_sem)
    coarse_out.start()

    f1[...] = r1.reshape(768, 128)[...].astype(F32)
    f2[...] = r2.reshape(512, 128)[...].astype(F32)
    f3[...] = r3.reshape(768, 128)[...].astype(F32)
    fc[...] = rc.reshape(256, 128)[...].astype(F32)
    cf[pl.ds(0, 128), :] = fc[pl.ds(0, 128, stride=2), :]
    cf[pl.ds(128, 32), :] = fc[pl.ds(65, 32, stride=2), :]
    for i in range(10):
        if i < 4:
            f = f2[pl.ds(i, 128, stride=4), :]
        else:
            f = f3[pl.ds(i - 4, 128, stride=6), :]
        med = f1[pl.ds(i % 5 + 6 * (i // 5), 64, stride=12), :]
        coarse = cf[pl.ds(i, 16, stride=10), :]
        f = jnp.concatenate([f[:16] + (med[:16] + coarse), f[16:64] + med[16:], f[64:]], axis=0)
        if i == 0:
            row = lax.broadcasted_iota(jnp.int32, (128, 128), 0)
            f = jnp.where(row == 0, f, 2.0 * f)
        else:
            f = 2.0 * f
        t = f.T.astype(BF16)
        x[pl.ds(i * 64, 64), pl.ds(0, 128)] = t[:64]
        x[pl.ds(i * 64, 64), pl.ds(128, 128)] = t[64:]
    y[...] = jnp.dot(x[...], w[...], preferred_element_type=F32)
    view = pv.reshape(20 * 64, 1, 128)
    for half in range(2):
        for j in range(5):
            col = pl.ds(j * 256 + half * 128, 128)
            parts = [None, None]
            for i in range(10):
                yr = y[pl.ds(i * 64, 64), pl.ds(half * 128, 128)]
                if i == 0:
                    term = yr
                else:
                    yi = y[pl.ds(i * 64, 64), pl.ds(256 + half * 128, 128)]
                    term = tw[pl.ds(i, 1), col] * yr - tw[pl.ds(16 + i, 1), col] * yi
                k = i % 2
                parts[k] = term if parts[k] is None else parts[k] + term
            for k, val in ((0, parts[0] + parts[1]), (5, parts[0] - parts[1])):
                lt = (j + k) * 2 + half
                pv[pl.ds(lt * 64, 64), :] = jnp.tanh(val)
                pltpu.make_async_copy(view.at[pl.ds(lt * 64, 64)], pat.at[:, :, pl.ds(lt * 128, 128)], p_sem).start()
    pltpu.make_async_copy(s_buf, s_buf, o_sem).wait()
    coarse_out.wait()
    pltpu.make_async_copy(pv, pv, p_sem).wait()


def synthesis_call(*parts):
    p = np.arange(128)[:, None]
    ang = 2.0 * math.pi * ((p * np.arange(256)[None, :]) % 256) / 256.0
    c, s = np.cos(ang), np.sin(ang)
    w = jnp.asarray(np.block([[c, s], [-s, c]]), BF16)
    i = np.arange(16)[:, None]
    ang = 2.0 * math.pi * ((i * np.arange(1280)[None, :]) % NLON) / NLON
    tw = jnp.asarray(np.concatenate([np.cos(ang), np.sin(ang)]), F32)
    s = jax.ShapeDtypeStruct
    v = pltpu.VMEM
    return pl.pallas_call(
        synthesis_kernel,
        name="synthesis",
        out_shape=(
            s((NE, 10, 2, MF), F32),
            s((NE, 5, 2, MM), F32),
            s((1, 2, MC, MC), F32),
            s((NE, 1, NLON), F32),
        ),
        in_specs=[VMEM] * 8,
        out_specs=(HBM,) * 4,
        scratch_shapes=[
            v((768, 128), F32),
            v((512, 128), F32),
            v((768, 128), F32),
            v((256, 128), F32),
            v((160, 128), F32),
            v((640, 256), BF16),
            v((640, 512), F32),
            v((1280, 128), F32),
            pltpu.SemaphoreType.DMA(()),
            pltpu.SemaphoreType.DMA(()),
            pltpu.SemaphoreType.DMA(()),
        ],
        compiler_params=pltpu.CompilerParams(vmem_limit_bytes=20 * 2**20),
        cost_estimate=pl.CostEstimate(flops=10**8, bytes_accessed=10**7, transcendentals=0),
    )(*parts, w, tw)


def body(fs, fn, ms, mn, cs, cn, decay, amplitude, fb, mb, cb):
    fs, fn, ms, mn = (a.transpose(0, 2, 1, 3) for a in (fs, fn, ms, mn))
    big = [pltpu.with_memory_space_constraint(a, pltpu.HBM) for a in (fs, fn, ms, mn, fb, mb, cs, cn, cb, decay, amplitude)]
    parts = spectral_call(*big)
    fine_next, medium_next, coarse_next, pattern = synthesis_call(*parts)
    return (fine_next.transpose(0, 2, 1, 3), medium_next.transpose(0, 2, 1, 3), coarse_next, pattern)


def solution(mesh):
    both = ("scale", "lat")
    return jax.shard_map(
        body,
        mesh=mesh,
        in_specs=(
            P(None, None, both, None),
            P(None, None, both, None),
            P(None, None, both, None),
            P(None, None, both, None),
            P("lat", None, None, None),
            P("lat", None, None, None),
            P(),
            P(),
            P(both, None, None),
            P(both, None, None),
            P(both, None, None),
        ),
        out_specs=(
            P(None, None, both, None),
            P(None, None, both, None),
            P("lat", None, None, None),
            P(None, both, None),
        ),
        check_vma=False,
    )
```

```python
import math

import jax
import jax.numpy as jnp
import numpy as np
from jax import lax
from jax.experimental import pallas as pl
from jax.experimental.pallas import tpu as pltpu
from jax.sharding import PartitionSpec as P

LOGICAL = pl.DeviceIdType.LOGICAL
F32, BF16 = jnp.float32, jnp.bfloat16
HBM = pl.BlockSpec(memory_space=pltpu.HBM)
VMEM = pl.BlockSpec(memory_space=pltpu.VMEM)
MF, MM, MC, NLON, NE, NR = 1280, 640, 160, 2560, 64, 128
ND = 128
NT = (((1,), (1,)), ((), ()))


def my_place():
    return lax.axis_index("scale") * 64 + lax.axis_index("lat")


BLOCKS = [(2, 0), (0, 0), (0, 1), (1, 0), (1, 1)]


def targets():
    lat = lax.axis_index("lat")
    y = lax.axis_index("scale") * 2 + lax.rem(lax.div(lat, 2), 2)
    x, z, core = lax.div(lat, 16), lax.rem(lax.div(lat, 4), 4), lax.rem(lat, 2)
    low = []
    for dy in (2, 1, 3, 0):
        for dc in (1, 0):
            yy = lax.rem(y + dy, 4)
            low.append(lax.div(yy, 2) * 64 + lax.rem(yy, 2) * 2 + lax.rem(core + dc, 2))
    return x, z, low


def others(act):
    x, z, low = targets()
    for dx in (2, 1, 3, 0):
        xx = lax.rem(x + dx, 4) * 16

        @pl.loop(1, 5 if dx else 4)
        def _(t):
            high = xx + lax.rem(z + t, 4) * 4
            for part in low:
                act(high + part)

    for part in low[:-1]:
        act(x * 16 + z * 4 + part)


def some_others(act, k):
    x, z, low = targets()
    pairs = [(dx, dz) for dx in (2, 1, 3, 0) for dz in (2, 1, 3, 0)]
    for dx, dz in pairs[3 * k : 3 * k + 3 if k < 4 else 16]:
        high = lax.rem(x + dx, 4) * 16 + lax.rem(z + dz, 4) * 4
        for part in low if dx or dz else low[:-1]:
            act(high + part)


def send_all(me, src, dst, send, recv, here, k=None):
    def one(d):
        pltpu.make_async_remote_copy(
            src.at[d], dst.at[me], send, recv, device_id=d, device_id_type=LOGICAL
        ).start()

    if k is None or k == 0:
        pltpu.make_async_copy(src.at[me], dst.at[me], here).start()
    if k is None:
        others(one)
    else:
        some_others(one, k)


def wait_rows(ref, count, sem):
    part = ref.at[pl.ds(0, count)]
    pltpu.make_async_copy(part, part, sem).wait()


def spectral_kernel(
    fs, fn, ms, mn, fb, mb, cs, cn, cb, dec_in, amp_in,
    s_buf, c_next, r1, r2, r3, rc,
    n_buf, n_flat, fb_buf, mb_buf, a_buf, acc, stage1, stage2, stage3, g1, g2, g3, gc,
    cs_buf, cn_buf, cb_buf, pad, c_stage, c_msg, c_got,
    dec, amp, s_sem, n_sem, b_sem, c_sem, send, recv, here,
):
    me = my_place()
    scale = lax.axis_index("scale")

    coarse_in = (
        pltpu.make_async_copy(cs, cs_buf, c_sem.at[0]),
        pltpu.make_async_copy(cn, cn_buf, c_sem.at[1]),
        pltpu.make_async_copy(cb, cb_buf, c_sem.at[2]),
        pltpu.make_async_copy(dec_in, dec, c_sem.at[3]),
        pltpu.make_async_copy(amp_in, amp, c_sem.at[4]),
    )
    for copy in coarse_in:
        copy.start()

    barrier = pltpu.get_barrier_semaphore()

    others(lambda d: pl.semaphore_signal(barrier, inc=1, device_id=d, device_id_type=LOGICAL))

    basis = [
        pltpu.make_async_copy(fb.at[pl.ds(0, 5)], fb_buf.at[pl.ds(0, 5)], b_sem.at[0]),
        pltpu.make_async_copy(fb.at[pl.ds(5, 5)], fb_buf.at[pl.ds(5, 5)], b_sem.at[1]),
        pltpu.make_async_copy(mb, mb_buf, b_sem.at[2]),
    ]
    started = set()
    for u, (grp, q) in enumerate(BLOCKS):
        for kt in range(5):
            lanes = pl.ds((q * 5 + kt) * 128, 128)
            rows = s_buf.at[u].reshape(5 * 64, 5, 2, 128).at[pl.ds(kt * 64, 64)]
            if grp == 2:
                src, nsrc, mid = ms, mn, slice(None)
            else:
                src, nsrc, mid = fs, fn, pl.ds(grp * 5, 5)
            pltpu.make_async_copy(src.at[:, mid, :, lanes], rows, s_sem.at[u]).start()
            pltpu.make_async_copy(nsrc.at[:, mid, :, lanes], n_buf.at[u, pl.ds(kt * 64, 64)], n_sem.at[u]).start()
        if grp not in started:
            started.add(grp)
            basis[grp].start()

    for copy in coarse_in:
        copy.wait()
    cdeg = lax.broadcasted_iota(jnp.int32, (MC, MC), 0) + lax.broadcasted_iota(jnp.int32, (MC, MC), 1)
    for c in range(2):
        val = dec[2] * cs_buf[0, c] + amp[2] * cn_buf[0, c].astype(F32)
        c_next[0, c] = jnp.where(cdeg < MC, val, 0.0)
    pad[...] = jnp.zeros_like(pad)
    pad[0, :, pl.ds(0, MC)] = c_next[0, scale]
    pad[1, :, pl.ds(0, MC)] = cb_buf[0].astype(F32)
    for k in range(2):
        c_stage[pl.ds(2 * k, 128, stride=4), :] = pad[k, pl.ds(0, 128), pl.ds(0, 128)]
        extra = jnp.concatenate(
            [pad[k, pl.ds(0, 32), pl.ds(128, 128)], pad[k, pl.ds(128, 32), pl.ds(0, 128)], jnp.zeros((64, 128), F32)], axis=0
        )
        c_stage[pl.ds(2 * k + 1, 128, stride=4), :] = extra
    c_msg.reshape(512, 128)[...] = c_stage[...].astype(BF16)

    rows40 = lax.broadcasted_iota(jnp.int32, (40, 128), 0)
    deg = lax.div(lax.rem(rows40, 10), 2) + lax.broadcasted_iota(jnp.int32, (40, 128), 1)

    def advance(u, kt):
        grp, q = BLOCKS[u]
        which = 1 if grp == 2 else 0
        size = MM if grp == 2 else MF
        first = me * 5 if grp == 2 else me * 10 + grp * 5
        d, a = dec[which], amp[which]
        inside = deg < size - first - (q * 5 + kt) * 128
        inside = jnp.concatenate([inside, inside], axis=0)
        noise = n_buf.at[u].reshape(3200, 128)
        for j in range(8):
            r = pl.ds(kt * 640 + j * 80, 80)
            n_flat[pl.ds(j * 80, 80), :] = noise[r, :]
            val = d * s_buf[u, r, :] + a * n_flat[pl.ds(j * 80, 80), :].astype(F32)
            s_buf[u, r, :] = jnp.where(inside, val, 0.0)
        for m in range(5):
            for c in range(2):
                v = s_buf[u, pl.ds(kt * 640 + m * 2 + c, 64, stride=10), :]
                a_buf[u % 2, m, pl.ds(c * 64, 64), pl.ds(kt * 128, 128)] = v.astype(BF16)

    def legendre(u, m):
        grp, q = BLOCKS[u]
        b = mb_buf[m] if grp == 2 else fb_buf[grp * 5 + m, :, pl.ds(q * 640, 640)]
        out = lax.dot_general(b, a_buf[u % 2, m], NT, preferred_element_type=F32)
        if grp < 2 and q == 0:
            acc[m] = out
        else:
            put[u](m, out + acc[m] if grp < 2 else out)

    def run(u, store=None, sends=None):
        if u < 5:
            pltpu.make_async_copy(s_buf.at[u], s_buf.at[u], s_sem.at[u]).wait()
            pltpu.make_async_copy(n_buf.at[u], n_buf.at[u], n_sem.at[u]).wait()
        if u > 0 and BLOCKS[u - 1][1] == 0:
            basis[BLOCKS[u - 1][0]].wait()
        for k in range(5):
            if sends is not None:
                sends(k)
            if u > 0:
                for m in ((0, 1), (2, 3), (4,), (), ())[k]:
                    legendre(u - 1, m)
            if u < 5:
                advance(u, k)
            if k == 2 and store is not None:
                store()

    def put_medium(m, out):
        stage1[pl.ds(m, 128, stride=6), :] = out

    def put_first(m, out):
        if m < 4:
            stage2[pl.ds(m, 128, stride=4), :] = out
        else:
            stage3[pl.ds(0, 128, stride=6), :] = out

    def put_last(m, out):
        stage3[pl.ds(1 + m, 128, stride=6), :] = out

    def store1():
        g1.reshape(768, 128)[...] = stage1[...].astype(BF16)

    def store2():
        g2.reshape(512, 128)[...] = stage2[...].astype(BF16)

    put = {0: put_medium, 2: put_first, 4: put_last}
    stage1[pl.ds(5, 128, stride=6), :] = jnp.zeros((128, 128), F32)
    run(0)
    run(1, store1)
    pl.semaphore_wait(barrier, ND - 1)
    run(2, None, lambda k: send_all(me, c_msg, c_got, send.at[3], recv.at[3], here.at[3], k))
    run(3, store2, lambda k: send_all(me, g1, r1, send.at[0], recv.at[0], here.at[0], k))
    run(4, None, lambda k: send_all(me, g2, r2, send.at[1], recv.at[1], here.at[1], k))
    run(5)
    g3.reshape(768, 128)[...] = stage3[...].astype(BF16)
    send_all(me, g3, r3, send.at[2], recv.at[2], here.at[2])

    wait_rows(c_got, ND - 1, recv.at[3])
    pltpu.make_async_copy(c_got.at[me], c_got.at[me], here.at[3]).wait()
    c_stage[...] = c_got.reshape(512, 128)[...].astype(F32)
    part = [c_stage[pl.ds(k, 128, stride=4), :].astype(BF16) for k in range(4)]
    main = lax.dot_general(part[2], part[0], NT, preferred_element_type=F32)
    extra = lax.dot_general(part[3], part[1], NT, preferred_element_type=F32)
    c_stage[pl.ds(0, 128, stride=2), :] = main + jnp.where(me < 32, extra, 0.0)
    c_stage[pl.ds(1, 128, stride=2), :] = extra
    gc.reshape(256, 128)[...] = c_stage[pl.ds(0, 256), :].astype(BF16)
    send_all(me, gc, rc, send.at[4], recv.at[4], here.at[4])

    wait_rows(c_got, ND - 1, send.at[3])
    for k, r in enumerate((r1, r2, r3)):
        pltpu.make_async_copy(r.at[0], r.at[0], here.at[k]).wait()
        wait_rows(r, ND - 1, send.at[k])
        wait_rows(r, ND - 1, recv.at[k])
    pltpu.make_async_copy(rc.at[0], rc.at[0], here.at[4]).wait()
    wait_rows(rc, ND - 1, send.at[4])
    wait_rows(rc, ND - 1, recv.at[4])


def spectral_call(fs, fn, ms, mn, fb, mb, cs, cn, cb, dec, amp):
    dma = pltpu.SemaphoreType.DMA
    v = pltpu.VMEM
    return pl.pallas_call(
        spectral_kernel,
        name="spectral",
        out_shape=(
            v((5, 3200, 128), F32),
            v((1, 2, MC, MC), F32),
            v((ND, 3, 2, 128), BF16),
            v((ND, 2, 2, 128), BF16),
            v((ND, 3, 2, 128), BF16),
            v((ND, 2, 128), BF16),
        ),
        in_specs=[HBM] * 11,
        out_specs=(VMEM,) * 6,
        scratch_shapes=[
            v((5, 320, 5, 2, 128), BF16),
            v((640, 128), BF16),
            v((10, 128, MF), BF16),
            v((5, 128, MM), BF16),
            v((2, 5, 128, 640), BF16),
            v((5, 128, 128), F32),
            v((768, 128), F32),
            v((512, 128), F32),
            v((768, 128), F32),
            v((ND, 3, 2, 128), BF16),
            v((ND, 2, 2, 128), BF16),
            v((ND, 3, 2, 128), BF16),
            v((ND, 2, 128), BF16),
            v((1, 2, MC, MC), F32),
            v((1, 2, MC, MC), BF16),
            v((1, MC, MC), BF16),
            v((2, MC, 256), F32),
            v((512, 128), F32),
            v((ND, 4, 128), BF16),
            v((ND, 4, 128), BF16),
            pltpu.SMEM((3,), F32),
            pltpu.SMEM((3,), F32),
            dma((5,)),
            dma((5,)),
            dma((3,)),
            dma((5,)),
            dma((5,)),
            dma((5,)),
            dma((5,)),
        ],
        compiler_params=pltpu.CompilerParams(has_side_effects=True, collective_id=0, vmem_limit_bytes=30 * 2**20),
        cost_estimate=pl.CostEstimate(flops=10**9, bytes_accessed=25 * 10**6, transcendentals=0),
    )(fs, fn, ms, mn, fb, mb, cs, cn, cb, dec, amp)


def synthesis_kernel(s_buf, c_next, r1, r2, r3, rc, w, tw, fo, mo, co, pat, f1, f2, f3, fc, cf, x, y, pv, o_sem, c_sem, p_sem):
    for u, (grp, q) in enumerate(BLOCKS):
        for kt in range(5):
            rows = s_buf.at[u].reshape(5 * 64, 5, 2, 128).at[pl.ds(kt * 64, 64)]
            dst, mid = (mo, slice(None)) if grp == 2 else (fo, pl.ds(grp * 5, 5))
            pltpu.make_async_copy(rows, dst.at[:, mid, :, pl.ds((q * 5 + kt) * 128, 128)], o_sem).start()
    coarse_out = pltpu.make_async_copy(c_next, co, c_sem)
    coarse_out.start()

    f1[...] = r1.reshape(768, 128)[...].astype(F32)
    f2[...] = r2.reshape(512, 128)[...].astype(F32)
    f3[...] = r3.reshape(768, 128)[...].astype(F32)
    fc[...] = rc.reshape(256, 128)[...].astype(F32)
    cf[pl.ds(0, 128), :] = fc[pl.ds(0, 128, stride=2), :]
    cf[pl.ds(128, 32), :] = fc[pl.ds(65, 32, stride=2), :]
    for i in range(10):
        if i < 4:
            f = f2[pl.ds(i, 128, stride=4), :]
        else:
            f = f3[pl.ds(i - 4, 128, stride=6), :]
        med = f1[pl.ds(i % 5 + 6 * (i // 5), 64, stride=12), :]
        coarse = cf[pl.ds(i, 16, stride=10), :]
        f = jnp.concatenate([f[:16] + (med[:16] + coarse), f[16:64] + med[16:], f[64:]], axis=0)
        if i == 0:
            row = lax.broadcasted_iota(jnp.int32, (128, 128), 0)
            f = jnp.where(row == 0, f, 2.0 * f)
        else:
            f = 2.0 * f
        t = f.T.astype(BF16)
        x[pl.ds(i * 64, 64), pl.ds(0, 128)] = t[:64]
        x[pl.ds(i * 64, 64), pl.ds(128, 128)] = t[64:]
    y[...] = jnp.dot(x[...], w[...], preferred_element_type=F32)
    view = pv.reshape(20 * 64, 1, 128)
    for half in range(2):
        for j in range(5):
            col = pl.ds(j * 256 + half * 128, 128)
            parts = [None, None]
            for i in range(10):
                yr = y[pl.ds(i * 64, 64), pl.ds(half * 128, 128)]
                if i == 0:
                    term = yr
                else:
                    yi = y[pl.ds(i * 64, 64), pl.ds(256 + half * 128, 128)]
                    term = tw[pl.ds(i, 1), col] * yr - tw[pl.ds(16 + i, 1), col] * yi
                k = i % 2
                parts[k] = term if parts[k] is None else parts[k] + term
            for k, val in ((0, parts[0] + parts[1]), (5, parts[0] - parts[1])):
                lt = (j + k) * 2 + half
                pv[pl.ds(lt * 64, 64), :] = jnp.tanh(val)
                pltpu.make_async_copy(view.at[pl.ds(lt * 64, 64)], pat.at[:, :, pl.ds(lt * 128, 128)], p_sem).start()
    pltpu.make_async_copy(s_buf, s_buf, o_sem).wait()
    coarse_out.wait()
    pltpu.make_async_copy(pv, pv, p_sem).wait()


def synthesis_call(*parts):
    p = np.arange(128)[:, None]
    ang = 2.0 * math.pi * ((p * np.arange(256)[None, :]) % 256) / 256.0
    c, s = np.cos(ang), np.sin(ang)
    w = jnp.asarray(np.block([[c, s], [-s, c]]), BF16)
    i = np.arange(16)[:, None]
    ang = 2.0 * math.pi * ((i * np.arange(1280)[None, :]) % NLON) / NLON
    tw = jnp.asarray(np.concatenate([np.cos(ang), np.sin(ang)]), F32)
    s = jax.ShapeDtypeStruct
    v = pltpu.VMEM
    return pl.pallas_call(
        synthesis_kernel,
        name="synthesis",
        out_shape=(
            s((NE, 10, 2, MF), F32),
            s((NE, 5, 2, MM), F32),
            s((1, 2, MC, MC), F32),
            s((NE, 1, NLON), F32),
        ),
        in_specs=[VMEM] * 8,
        out_specs=(HBM,) * 4,
        scratch_shapes=[
            v((768, 128), F32),
            v((512, 128), F32),
            v((768, 128), F32),
            v((256, 128), F32),
            v((160, 128), F32),
            v((640, 256), BF16),
            v((640, 512), F32),
            v((1280, 128), F32),
            pltpu.SemaphoreType.DMA(()),
            pltpu.SemaphoreType.DMA(()),
            pltpu.SemaphoreType.DMA(()),
        ],
        compiler_params=pltpu.CompilerParams(vmem_limit_bytes=20 * 2**20),
        cost_estimate=pl.CostEstimate(flops=10**8, bytes_accessed=10**7, transcendentals=0),
    )(*parts, w, tw)


def body(fs, fn, ms, mn, cs, cn, decay, amplitude, fb, mb, cb):
    fs, fn, ms, mn = (a.transpose(0, 2, 1, 3) for a in (fs, fn, ms, mn))
    big = [pltpu.with_memory_space_constraint(a, pltpu.HBM) for a in (fs, fn, ms, mn, fb, mb, cs, cn, cb, decay, amplitude)]
    parts = spectral_call(*big)
    fine_next, medium_next, coarse_next, pattern = synthesis_call(*parts)
    return (fine_next.transpose(0, 2, 1, 3), medium_next.transpose(0, 2, 1, 3), coarse_next, pattern)


def solution(mesh):
    both = ("scale", "lat")
    return jax.shard_map(
        body,
        mesh=mesh,
        in_specs=(
            P(None, None, both, None),
            P(None, None, both, None),
            P(None, None, both, None),
            P(None, None, both, None),
            P("lat", None, None, None),
            P("lat", None, None, None),
            P(),
            P(),
            P(both, None, None),
            P(both, None, None),
            P(both, None, None),
        ),
        out_specs=(
            P(None, None, both, None),
            P(None, None, both, None),
            P("lat", None, None, None),
            P(None, both, None),
        ),
        check_vma=False,
    )
```
